32 devices in a mesh: row: 4 (over z), col: 8 (over y, x, core).
Axes of the slice: x: 2, y: 2, z: 4, core: 2. Of those that a mesh axis runs over, the one named last changes fastest.
Arguments:
- pressure: float32 [128, 256, 512], P('row', 'col'), may hold values from -6 to 6
- cut_exponent: int32 [4, 8, 2], P('row', 'col'), may hold values from 0 to 3
- group_map: int32 [4, 8, 2], P('row', 'col'), may hold values from 0 to 15
Outputs:
- coeffs: float32 [128, 256, 512], P('row', 'col')
- group_mass: float32 [16, 4], replicated
The draws below stay inside these ranges and needn't reach their ends.
Inputs may be any that keep to these rules, and one draw needn't show every extreme that they name: `cut_exponent`: one exponent per block of 32 x 32 x 512 // 2 cells.
All inputs are finite; a program needn't handle non-finite values.
Results may differ from the reference program's by a relative error of at most 0.0001.
Values sent between devices are 32-bit elements; how exact they have to be, the bound alone decides.
A program may use at most 64 MiB of HBM per device.

```python
import jax
import jax.numpy as jnp
from jax import lax

CX = 32
CY = 32
CZ = 512
ZB = 2
GROUPS = 16
NX = 128
NY = 256
N_ROW = 4
N_COL = 8


def with_ends(entries, rng, low, largest):
    dims = entries.shape
    place = [jax.random.randint(jax.random.fold_in(rng, axis), (), 0, dims[axis]) for axis in range(len(dims))]
    entries = entries.at[tuple(place)].set(low)
    longest = dims.index(max(dims))
    place[longest] = (place[longest] + 1) % dims[longest]
    return entries.at[tuple(place)].set(largest)


def block_scale(rng, shape, cuts, low, largest):
    def one(axis_at, blocks):
        steps = jax.random.uniform(jax.random.fold_in(jax.random.fold_in(rng, 6), axis_at), (blocks,), jnp.float32, low / len(cuts), largest / len(cuts))
        return jnp.repeat(jnp.exp(steps), shape[axis_at] // blocks).reshape((-1,) + (1,) * (len(shape) - axis_at - 1))

    gain = one(*cuts[0])
    for cut in cuts[1:]:
        gain = gain * one(*cut)
    return gain


def bell_draw(stream_key, shape, spread, most, cuts=(), held_as=jnp.bfloat16):
    values = jax.random.normal(stream_key, shape, jnp.float32) * spread
    if len(cuts) > 0:
        values = block_scale(stream_key, shape, cuts, -0.22, 0.18) * values
    return jnp.clip(values, min=-most, max=most).astype(held_as)


def setup_inputs(seed: int = 0) -> dict:
    splits = jax.random.split(jax.random.key(seed), 4)
    pressure = bell_draw(splits[0], (NX, NY, CZ), 1.0, 6.0, ((0, 4), (1, 8)), jnp.float32)
    cut_exponent = with_ends(jax.random.randint(splits[1], (N_ROW, N_COL, ZB), 0, 4), jax.random.fold_in(splits[1], 1), 0, 3).astype(jnp.int32)
    group_map = with_ends(jax.random.randint(splits[2], (N_ROW, N_COL, ZB), 0, GROUPS), jax.random.fold_in(splits[2], 1), 0, GROUPS - 1).astype(jnp.int32)
    return dict(pressure=pressure, cut_exponent=cut_exponent, group_map=group_map)


cut_levels = (0.25, 0.5, 1.0, 2.0)


def lift_axis(signal, axis_pos):
    length = signal.shape[axis_pos]
    evens_half = lax.slice_in_dim(signal, 0, length, stride=2, axis=axis_pos)
    odds_half = lax.slice_in_dim(signal, 1, length, stride=2, axis=axis_pos)
    guess = 0.5625 * (evens_half + jnp.roll(evens_half, -1, axis_pos)) - 0.0625 * (jnp.roll(evens_half, 1, axis_pos) + jnp.roll(evens_half, -2, axis_pos))
    detail = odds_half - guess
    smooth = evens_half + (0.28125 * (jnp.roll(detail, 1, axis_pos) + detail) - 0.03125 * (jnp.roll(detail, 2, axis_pos) + jnp.roll(detail, -1, axis_pos)))
    return jnp.stack([smooth, detail], axis_pos + 1).reshape(signal.shape)


def reference(pressure, cut_exponent, group_map):
    coeffs = lift_axis(pressure, 0)
    coeffs = lift_axis(coeffs, 1)
    coeffs = lift_axis(coeffs, 2)
    parity_x = (jnp.arange(NX, dtype=jnp.int32) % 2)[:, None, None]
    parity_y = (jnp.arange(NY, dtype=jnp.int32) % 2)[None, :, None]
    parity_z = (jnp.arange(CZ, dtype=jnp.int32) % 2)[None, None, :]
    detail_mask = (parity_x + parity_y + parity_z) > 0
    magnitude = jnp.where(detail_mask, jnp.abs(coeffs), jnp.float32(0.0))
    shaped = magnitude.reshape(N_ROW, CX, N_COL, CY, ZB, CZ // ZB)
    scales = jnp.exp2(-cut_exponent.astype(jnp.float32))
    cells = CX * CY * (CZ // ZB)
    block_list = []
    for level_value in cut_levels:
        limit = (level_value * scales)[:, None, :, None, :, None]
        block_list.append(jnp.sum(jnp.maximum(shaped - limit, 0.0), axis=(1, 3, 5)) / cells)
    block_mass = jnp.stack(block_list, -1)
    onehot = (group_map[..., None] == jnp.arange(GROUPS, dtype=jnp.int32)).astype(jnp.float32)
    group_mass = jnp.einsum("abzg,abzk->gk", onehot, block_mass.astype(jnp.float32), precision=lax.Precision.HIGHEST)
    return coeffs, group_mass
```

```python
import functools

import jax
import jax.numpy as jnp
import numpy as np
from jax import lax
from jax.experimental import pallas as pl
from jax.experimental.pallas import tpu as pltpu
from jax.sharding import PartitionSpec as P

GROUPS = 16
LEVELS = (0.25, 0.5, 1.0, 2.0)
MESH = pl.DeviceIdType.MESH
F32, BF16 = jnp.float32, jnp.bfloat16


def cyclic_matrix(n):
    half = n // 2
    ev, od = np.eye(n)[0::2], np.eye(n)[1::2]
    r = lambda a, k: np.roll(a, k, 0)
    d = od - (0.5625 * (ev + r(ev, -1)) - 0.0625 * (r(ev, 1) + r(ev, -2)))
    s = ev + (0.28125 * (r(d, 1) + d) - 0.03125 * (r(d, 2) + r(d, -1)))
    return np.stack([s, d], 1).reshape(n, n) if half else None


def local_matrix(n):
    half = n // 2
    t = np.eye(n + 6)
    v, (a, b, c, f0, f1, g) = t[:n], t[n:]
    e = {j: v[2 * j] for j in range(half)}
    o = {j: v[2 * j + 1] for j in range(half)}
    e[-1], e[half], e[half + 1] = a, f0, f1
    d = {
        j: o[j] - 0.5625 * (e[j] + e[j + 1]) + 0.0625 * (e[j - 1] + e[j + 2])
        for j in range(half)
    }
    d[-1] = b - 0.5625 * e[0] + 0.0625 * e[1]
    d[-2] = c + 0.0625 * e[0]
    d[half] = g + 0.0625 * e[half - 1]
    out = np.zeros((n, n + 6))
    for j in range(half):
        out[2 * j] = e[j] + 0.28125 * (d[j - 1] + d[j]) - 0.03125 * (d[j - 2] + d[j + 1])
        out[2 * j + 1] = d[j]
    return out


def partials_low(row, n):
    a = row(n - 2)
    b = row(n - 1) - 0.5625 * a + 0.0625 * row(n - 4)
    c = row(n - 3) - 0.5625 * (row(n - 4) + a) + 0.0625 * row(n - 6)
    return a, b, c


def partials_high(row):
    f0, f1 = row(0), row(2)
    return f0, f1, row(1) - 0.5625 * (f0 + f1) + 0.0625 * row(4)


def split(value):
    hi = value.astype(BF16)
    return hi, (value - hi.astype(F32)).astype(BF16)


def dot2(left, right):
    dot = functools.partial(jnp.dot, preferred_element_type=F32)
    if left.dtype == BF16:
        hi, lo = split(right)
        return dot(left, hi) + dot(left, lo)
    hi, lo = split(left)
    return dot(hi, right) + dot(lo, right)


def kernel(
    n_row, n_col, grp, cut_ref, map_ref, p_ref, ws_ref, wy_ref, wu_ref, wx_ref, wc_ref, wz_ref,
    out_ref, mass_ref,
    ext, q, sx, su, u, sc, cb, part, slots,
    in_sem, h_send, h_recv, g_send, g_recv,
):
    nx, ny, nz = p_ref.shape
    devices = n_row * n_col
    row, col = lax.axis_index("row"), lax.axis_index("col")
    me = row * n_col + col
    up_r, dn_r = lax.rem(row + 1, n_row), lax.rem(row + n_row - 1, n_row)
    up_c, dn_c = lax.rem(col + 1, n_col), lax.rem(col + n_col - 1, n_col)

    pieces = ((0, 8), (nx - 8, 8), (8, nx - 16))
    loads = []
    for i, (at, size) in enumerate(pieces):
        load = pltpu.make_async_copy(
            p_ref.at[pl.ds(at, size)], ext.at[pl.ds(at, size)], in_sem.at[i]
        )
        load.start()
        loads.append(load)

    def place(k):
        t = lax.rem(me + k, devices)
        return (t // n_col, lax.rem(t, n_col))

    barrier = pltpu.get_barrier_semaphore()

    @pl.loop(1, devices)
    def _(k):
        pl.semaphore_signal(barrier, inc=1, device_id=place(k), device_id_type=MESH)

    sends = []

    def send(src, dst, to):
        i = len(sends)
        copy = pltpu.make_async_remote_copy(
            src_ref=src, dst_ref=dst, send_sem=h_send.at[i], recv_sem=h_recv.at[i],
            device_id=to, device_id_type=MESH,
        )
        copy.start()
        sends.append(copy)

    loads[0].wait()
    loads[1].wait()
    _, b, c = partials_low(lambda i: ext[i], nx)
    sx[0], sx[1] = b, c
    sx[2] = partials_high(lambda i: ext[i])[2]
    loads[2].wait()
    for g in range(nx // grp):
        at = pl.ds(g * grp, grp)
        got = dot2(ws_ref[...], ext[at].reshape(grp * ny, nz))
        su[:, at, :] = got.reshape(6, grp, nz)
    sc[...] = jnp.zeros_like(sc)
    for d in range(4):
        for k in range(3):
            plane = (d % 2) * 3 + k
            x_row = lambda i: su[plane, pl.ds(i, 1), :]
            got = partials_low(x_row, nx) if d < 2 else partials_high(x_row)
            for i in range(3):
                sc[d, pl.ds(3 * i + k, 1), :] = got[i]

    pl.semaphore_wait(barrier, devices - 1)
    send(ext.at[nx - 2], ext.at[nx], (up_r, col))
    send(ext.at[0], ext.at[nx + 3], (dn_r, col))
    send(ext.at[2], ext.at[nx + 4], (dn_r, col))
    send(su.at[pl.ds(0, 3)], u.at[pl.ds(0, 3)], (row, up_c))
    send(su.at[pl.ds(3, 3)], u.at[pl.ds(3, 3)], (row, dn_c))
    send(sx.at[pl.ds(0, 2)], ext.at[pl.ds(nx + 1, 2)], (up_r, col))
    send(sx.at[2], ext.at[nx + 5], (dn_r, col))
    for d in range(4):
        to = (up_r if d < 2 else dn_r, up_c if d % 2 == 0 else dn_c)
        send(sc.at[d], cb.at[d], to)

    for g in range(nx // grp):
        at = pl.ds(g * grp, grp)
        q[at] = dot2(wy_ref[...], ext[at].reshape(grp * ny, nz)).reshape(grp, ny, nz)
    for copy in sends:
        copy.wait_recv()
    for g in range(nx // grp):
        at = pl.ds(g * grp, grp)
        more = dot2(wu_ref[...], u[:, at, :].reshape(6 * grp, nz))
        q[at] += more.reshape(grp, ny, nz)
    edge = dot2(wx_ref[...], ext[pl.ds(nx, 6)].reshape(6 * ny, nz))
    edge += dot2(wc_ref[...], cb[...].reshape(-1, nz))
    q[pl.ds(nx, 6)] = edge.reshape(6, ny, nz)

    for copy in sends:
        copy.wait_send()
    half = nx // 2

    @pl.loop(0, ny // 8)
    def _(t):
        rows = pl.ds(pl.multiple_of(t * 8, 8), 8)
        e = {j: q[2 * j, rows, :] for j in range(-0, half)}
        o = lambda j: q[2 * j + 1, rows, :]
        e[-1], e[half], e[half + 1] = (q[nx + i, rows, :] for i in (0, 3, 4))
        d = {
            -1: q[nx + 1, rows, :] - 0.5625 * e[0] + 0.0625 * e[1],
            -2: q[nx + 2, rows, :] + 0.0625 * e[0],
        }

        def detail(j):
            if j == half:
                return q[nx + 5, rows, :] + 0.0625 * e[half - 1]
            return o(j) - 0.5625 * (e[j] + e[j + 1]) + 0.0625 * (e[j - 1] + e[j + 2])

        d[0] = detail(0)
        for j in range(half):
            d[j + 1] = detail(j + 1)
            smooth = e[j] + 0.28125 * (d[j - 1] + d[j]) - 0.03125 * (d[j - 2] + d[j + 1])
            ext[2 * j, rows, :] = smooth
            ext[2 * j + 1, rows, :] = d[j]

    zb = cut_ref.shape[2]
    width = nz // zb
    cuts = jnp.concatenate(
        [jnp.full((1, width), -cut_ref[0, 0, z], jnp.int32) for z in range(zb)], 1
    )
    scale = jnp.exp2(cuts.astype(F32))
    limits = [level * scale for level in LEVELS]
    odd = lambda axis: lax.broadcasted_iota(jnp.int32, (8, nz), axis) % 2
    mixed = (odd(0) + odd(1)) > 0

    def z_group(g, totals):
        at = pl.ds(g * grp, grp)
        made = dot2(ext[at].reshape(grp * ny, nz), wz_ref[...])
        out_ref[at] = made.reshape(grp, ny, nz)
        totals = list(totals)
        for i in range(grp * ny // 8):
            size = jnp.abs(made[8 * i : 8 * i + 8])
            if (8 * i // ny) % 2 == 0:
                size = jnp.where(mixed, size, 0.0)
            for n, limit in enumerate(limits):
                totals[n] += jnp.maximum(size - limit, 0.0)
        return tuple(totals)

    totals = lax.fori_loop(
        0, nx // grp, z_group, tuple(jnp.zeros((8, nz), F32) for _ in LEVELS)
    )
    lane = lax.broadcasted_iota(jnp.int32, (1, 128), 1)
    line = jnp.zeros((1, 128), F32)
    cells = nx * ny * width
    n_lev = len(LEVELS)
    for z in range(zb):
        for n in range(n_lev):
            mass = jnp.sum(totals[n][:, z * width : (z + 1) * width], keepdims=True) / cells
            line += jnp.where(lane == map_ref[0, 0, z] * n_lev + n, mass, 0.0)
    part[...] = line
    slots[me] = line

    def spread(k):
        t = lax.rem(me + k, devices)
        return pltpu.make_async_remote_copy(
            src_ref=part, dst_ref=slots.at[me], send_sem=g_send.at[t],
            recv_sem=g_recv.at[me], device_id=place(k), device_id_type=MESH,
        )

    @pl.loop(1, devices)
    def _(k):
        spread(k).start()

    @pl.loop(1, devices)
    def _(k):
        t = lax.rem(me + k, devices)
        pltpu.make_async_remote_copy(
            src_ref=part, dst_ref=slots.at[t], send_sem=g_send.at[t],
            recv_sem=g_recv.at[t], device_id=place(k), device_id_type=MESH,
        ).wait()

    total = jnp.sum(slots[...], axis=0)
    wide = jnp.broadcast_to(total, (GROUPS, 128))
    at_row = lax.broadcasted_iota(jnp.int32, (GROUPS, 128), 0)
    at_lane = lax.broadcasted_iota(jnp.int32, (GROUPS, 128), 1)
    at_col = lax.broadcasted_iota(jnp.int32, (GROUPS, n_lev), 1)
    result = jnp.zeros((GROUPS, n_lev), F32)
    for n in range(n_lev):
        pick = jnp.where(at_lane == at_row * n_lev + n, wide, 0.0)
        result = jnp.where(at_col == n, jnp.sum(pick, axis=1, keepdims=True), result)
    mass_ref[...] = result


def solution(mesh):
    n_row, n_col = mesh.shape["row"], mesh.shape["col"]

    def shards(pressure, cut_exponent, group_map):
        nx, ny, nz = pressure.shape
        grp = 8
        devices = n_row * n_col
        local = local_matrix(ny)
        wy = np.kron(np.eye(grp), local[:, :ny])
        wu = np.einsum("xw,yk->xykw", np.eye(grp), local[:, ny:]).reshape(grp * ny, 6 * grp)
        eye = np.eye(ny)
        row = lambda i: eye[i]
        near = np.stack(partials_low(row, ny) + partials_high(row))
        ws = np.einsum("ky,xw->kxwy", near, np.eye(grp)).reshape(6 * grp, grp * ny)
        wx = np.kron(np.eye(6), local[:, :ny])
        wc = np.zeros((6, ny, 4, 16))
        for d in range(4):
            for i in range(3):
                for k in range(3):
                    wc[(d // 2) * 3 + i, :, d, 3 * i + k] = local[:, ny + (d % 2) * 3 + k]
        wc = wc.reshape(6 * ny, 64)
        weights = [jnp.asarray(w, BF16) for w in (ws, wy, wu, wx, wc, cyclic_matrix(nz).T)]
        vmem = pl.BlockSpec(memory_space=pltpu.VMEM)
        smem = pl.BlockSpec(memory_space=pltpu.SMEM)
        return pl.pallas_call(
            functools.partial(kernel, n_row, n_col, grp),
            out_shape=(
                jax.ShapeDtypeStruct((nx, ny, nz), F32),
                jax.ShapeDtypeStruct((GROUPS, len(LEVELS)), F32),
            ),
            in_specs=[smem, smem, pl.BlockSpec(memory_space=pltpu.HBM)] + [vmem] * 6,
            out_specs=(vmem, vmem),
            scratch_shapes=[
                pltpu.VMEM((nx + 8, ny, nz), F32),
                pltpu.VMEM((nx + 6, ny, nz), F32),
                pltpu.VMEM((3, ny, nz), F32),
                pltpu.VMEM((6, nx, nz), F32),
                pltpu.VMEM((6, nx, nz), F32),
                pltpu.VMEM((4, 16, nz), F32),
                pltpu.VMEM((4, 16, nz), F32),
                pltpu.VMEM((1, 128), F32),
                pltpu.VMEM((devices, 1, 128), F32),
                pltpu.SemaphoreType.DMA((3,)),
                pltpu.SemaphoreType.DMA((11,)),
                pltpu.SemaphoreType.DMA((11,)),
                pltpu.SemaphoreType.DMA((devices,)),
                pltpu.SemaphoreType.DMA((devices,)),
            ],
            compiler_params=pltpu.CompilerParams(
                collective_id=0, has_side_effects=True, vmem_limit_bytes=28 * 2**20
            ),
        )(cut_exponent, group_map, pressure, *weights)

    specs = P("row", "col", None)
    return jax.shard_map(
        shards, mesh=mesh, in_specs=(specs,) * 3, out_specs=(specs, P()), check_vma=False
    )
```

```python
import functools

import jax
import jax.numpy as jnp
import numpy as np
from jax import lax
from jax.experimental import pallas as pl
from jax.experimental.pallas import tpu as pltpu
from jax.sharding import PartitionSpec as P

GROUPS = 16
LEVELS = (0.25, 0.5, 1.0, 2.0)
MESH = pl.DeviceIdType.MESH
F32, BF16 = jnp.float32, jnp.bfloat16


def cyclic_matrix(n):
    half = n // 2
    ev, od = np.eye(n)[0::2], np.eye(n)[1::2]
    r = lambda a, k: np.roll(a, k, 0)
    d = od - (0.5625 * (ev + r(ev, -1)) - 0.0625 * (r(ev, 1) + r(ev, -2)))
    s = ev + (0.28125 * (r(d, 1) + d) - 0.03125 * (r(d, 2) + r(d, -1)))
    return np.stack([s, d], 1).reshape(n, n) if half else None


def local_matrix(n):
    half = n // 2
    t = np.eye(n + 6)
    v, (a, b, c, f0, f1, g) = t[:n], t[n:]
    e = {j: v[2 * j] for j in range(half)}
    o = {j: v[2 * j + 1] for j in range(half)}
    e[-1], e[half], e[half + 1] = a, f0, f1
    d = {
        j: o[j] - 0.5625 * (e[j] + e[j + 1]) + 0.0625 * (e[j - 1] + e[j + 2])
        for j in range(half)
    }
    d[-1] = b - 0.5625 * e[0] + 0.0625 * e[1]
    d[-2] = c + 0.0625 * e[0]
    d[half] = g + 0.0625 * e[half - 1]
    out = np.zeros((n, n + 6))
    for j in range(half):
        out[2 * j] = e[j] + 0.28125 * (d[j - 1] + d[j]) - 0.03125 * (d[j - 2] + d[j + 1])
        out[2 * j + 1] = d[j]
    return out


def partials_low(row, n):
    a = row(n - 2)
    b = row(n - 1) - 0.5625 * a + 0.0625 * row(n - 4)
    c = row(n - 3) - 0.5625 * (row(n - 4) + a) + 0.0625 * row(n - 6)
    return a, b, c


def partials_high(row):
    f0, f1 = row(0), row(2)
    return f0, f1, row(1) - 0.5625 * (f0 + f1) + 0.0625 * row(4)


def split(value):
    hi = value.astype(BF16)
    return hi, (value - hi.astype(F32)).astype(BF16)


def dot2(left, right):
    dot = functools.partial(jnp.dot, preferred_element_type=F32)
    if left.dtype == BF16:
        hi, lo = split(right)
        return dot(left, hi) + dot(left, lo)
    hi, lo = split(left)
    return dot(hi, right) + dot(lo, right)


def kernel(
    n_row, n_col, grp, cut_hbm, map_hbm, p_ref, *refs
):
    weights, refs = refs[:6], refs[6:]
    out_hbm, mass_ref = refs[:2]
    ext, q, sx, su, u, sc, cb, part, slots, out_ref, cut_ref, map_ref = refs[2:14]
    held = refs[14:20]
    ws_ref, wy_ref, wu_ref, wx_ref, wc_ref, wz_ref = held
    in_sem, o_sem, w_sem, h_send, h_recv, g_send, g_recv = refs[20:]
    nx, ny, nz = p_ref.shape
    devices = n_row * n_col
    row, col = lax.axis_index("row"), lax.axis_index("col")
    me = row * n_col + col
    up_r, dn_r = lax.rem(row + 1, n_row), lax.rem(row + n_row - 1, n_row)
    up_c, dn_c = lax.rem(col + 1, n_col), lax.rem(col + n_col - 1, n_col)

    pieces = ((0, 8), (nx - 8, 8), (8, nx - 16))
    loads = []
    for i, (at, size) in enumerate(pieces):
        load = pltpu.make_async_copy(
            p_ref.at[pl.ds(at, size)], ext.at[pl.ds(at, size)], in_sem.at[i]
        )
        load.start()
        loads.append(load)

    fetched = []
    for i, (src, dst) in enumerate(
        zip((*weights, cut_hbm, map_hbm), (*held, cut_ref, map_ref), strict=True)
    ):
        fetch = pltpu.make_async_copy(src, dst, w_sem.at[i])
        fetch.start()
        fetched.append(fetch)

    def place(k):
        t = lax.rem(me + k, devices)
        return (t // n_col, lax.rem(t, n_col))

    barrier = pltpu.get_barrier_semaphore()

    @pl.loop(1, devices)
    def _(k):
        pl.semaphore_signal(barrier, inc=1, device_id=place(k), device_id_type=MESH)

    sends = []

    def send(src, dst, to):
        i = len(sends)
        copy = pltpu.make_async_remote_copy(
            src_ref=src, dst_ref=dst, send_sem=h_send.at[i], recv_sem=h_recv.at[i],
            device_id=to, device_id_type=MESH,
        )
        copy.start()
        sends.append(copy)

    loads[0].wait()
    loads[1].wait()
    _, b, c = partials_low(lambda i: ext[i], nx)
    sx[0], sx[1] = b, c
    sx[2] = partials_high(lambda i: ext[i])[2]
    pl.semaphore_wait(barrier, devices - 1)
    send(sx.at[pl.ds(0, 2)], ext.at[pl.ds(nx + 1, 2)], (up_r, col))
    send(sx.at[2], ext.at[nx + 5], (dn_r, col))
    send(ext.at[nx - 2], ext.at[nx], (up_r, col))
    send(ext.at[0], ext.at[nx + 3], (dn_r, col))
    send(ext.at[2], ext.at[nx + 4], (dn_r, col))
    loads[2].wait()
    for fetch in fetched:
        fetch.wait()
    for g in range(nx // grp):
        at = pl.ds(g * grp, grp)
        got = dot2(ws_ref[...], ext[at].reshape(grp * ny, nz))
        su[:, at, :] = got.reshape(6, grp, nz)
    for d in range(4):
        for k in range(3):
            plane = (d % 2) * 3 + k
            x_row = lambda i: su[plane, pl.ds(i, 1), :]
            got = partials_low(x_row, nx) if d < 2 else partials_high(x_row)
            for i in range(3):
                sc[9 * d + 3 * i + k] = got[i]

    send(su.at[pl.ds(0, 3)], u.at[pl.ds(0, 3)], (row, up_c))
    send(su.at[pl.ds(3, 3)], u.at[pl.ds(3, 3)], (row, dn_c))
    for d in range(4):
        to = (up_r if d < 2 else dn_r, up_c if d % 2 == 0 else dn_c)
        send(sc.at[pl.ds(9 * d, 9)], cb.at[pl.ds(9 * d, 9)], to)

    for g in range(nx // grp):
        at = pl.ds(g * grp, grp)
        q[at] = dot2(wy_ref[...], ext[at].reshape(grp * ny, nz)).reshape(grp, ny, nz)
    for copy in sends[5:7]:
        copy.wait_recv()
    for g in range(nx // grp):
        at = pl.ds(g * grp, grp)
        more = dot2(wu_ref[...], u[:, at, :].reshape(6 * grp, nz))
        q[at] += more.reshape(grp, ny, nz)
    half = nx // 2

    def x_lift(low, high):
        @pl.loop(0, ny // 8)
        def _(t):
            rows = pl.ds(pl.multiple_of(t * 8, 8), 8)
            far = {-1: nx, half: nx + 3, half + 1: nx + 4}
            first, last = max(low - 3, -1), min(high + 2, half + 1)
            e = {j: q[far.get(j, 2 * j), rows, :] for j in range(first, last + 1)}

            def detail(j):
                if j == -1:
                    return q[nx + 1, rows, :] - 0.5625 * e[0] + 0.0625 * e[1]
                if j == -2:
                    return q[nx + 2, rows, :] + 0.0625 * e[0]
                if j == half:
                    return q[nx + 5, rows, :] + 0.0625 * e[half - 1]
                odd = q[2 * j + 1, rows, :]
                return odd - 0.5625 * (e[j] + e[j + 1]) + 0.0625 * (e[j - 1] + e[j + 2])

            d = {j: detail(j) for j in range(low - 2, low + 1)}
            for j in range(low, high):
                d[j + 1] = detail(j + 1)
                near, wide = d[j - 1] + d[j], d[j - 2] + d[j + 1]
                ext[2 * j, rows, :] = e[j] + 0.28125 * near - 0.03125 * wide
                ext[2 * j + 1, rows, :] = d[j]

    zb = cut_ref.shape[2]
    width = nz // zb
    cuts = jnp.concatenate(
        [jnp.full((1, width), -cut_ref[0, 0, z], jnp.int32) for z in range(zb)], 1
    )
    scale = jnp.exp2(cuts.astype(F32))
    limits = [level * scale for level in LEVELS]
    odd = lambda axis: lax.broadcasted_iota(jnp.int32, (8, nz), axis) % 2
    mixed = (odd(0) + odd(1)) > 0

    def z_group(g, totals):
        at = pl.ds(g * grp, grp)
        made = dot2(ext[at].reshape(grp * ny, nz), wz_ref[...])
        out_ref[at] = made.reshape(grp, ny, nz)
        pltpu.make_async_copy(out_ref.at[at], out_hbm.at[at], o_sem.at[g]).start()
        totals = list(totals)
        for i in range(grp * ny // 8):
            size = jnp.abs(made[8 * i : 8 * i + 8])
            if (8 * i // ny) % 2 == 0:
                size = jnp.where(mixed, size, 0.0)
            for n, limit in enumerate(limits):
                totals[n] += jnp.maximum(size - limit, 0.0)
        return tuple(totals)

    groups = nx // grp
    totals = tuple(jnp.zeros((8, nz), F32) for _ in LEVELS)
    x_lift(grp // 2, half - grp // 2)
    totals = lax.fori_loop(1, groups - 1, z_group, totals)
    for copy in sends[:5] + sends[7:]:
        copy.wait_recv()
    for copy in sends:
        copy.wait_send()
    edge = dot2(wx_ref[...], ext[pl.ds(nx, 6)].reshape(6 * ny, nz))
    edge += dot2(wc_ref[...], cb[...].reshape(-1, nz))
    q[pl.ds(nx, 6)] = edge.reshape(6, ny, nz)
    x_lift(0, grp // 2)
    x_lift(half - grp // 2, half)
    for g in (0, groups - 1):
        totals = z_group(g, totals)
    lane = lax.broadcasted_iota(jnp.int32, (1, 128), 1)
    line = jnp.zeros((1, 128), F32)
    cells = nx * ny * width
    n_lev = len(LEVELS)
    for z in range(zb):
        for n in range(n_lev):
            mass = jnp.sum(totals[n][:, z * width : (z + 1) * width], keepdims=True) / cells
            line += jnp.where(lane == map_ref[0, 0, z] * n_lev + n, mass, 0.0)
    part[...] = line
    slots[me] = line

    def spread(k):
        t = lax.rem(me + k, devices)
        return pltpu.make_async_remote_copy(
            src_ref=part, dst_ref=slots.at[me], send_sem=g_send.at[t],
            recv_sem=g_recv.at[me], device_id=place(k), device_id_type=MESH,
        )

    @pl.loop(1, devices)
    def _(k):
        spread(k).start()

    @pl.loop(1, devices)
    def _(k):
        t = lax.rem(me + k, devices)
        pltpu.make_async_remote_copy(
            src_ref=part, dst_ref=slots.at[t], send_sem=g_send.at[t],
            recv_sem=g_recv.at[t], device_id=place(k), device_id_type=MESH,
        ).wait()

    for g in range(groups):
        at = pl.ds(g * grp, grp)
        pltpu.make_async_copy(out_ref.at[at], out_hbm.at[at], o_sem.at[g]).wait()

    total = jnp.sum(slots[...], axis=0)
    wide = jnp.broadcast_to(total, (GROUPS, 128))
    at_row = lax.broadcasted_iota(jnp.int32, (GROUPS, 128), 0)
    at_lane = lax.broadcasted_iota(jnp.int32, (GROUPS, 128), 1)
    at_col = lax.broadcasted_iota(jnp.int32, (GROUPS, n_lev), 1)
    result = jnp.zeros((GROUPS, n_lev), F32)
    for n in range(n_lev):
        pick = jnp.where(at_lane == at_row * n_lev + n, wide, 0.0)
        result = jnp.where(at_col == n, jnp.sum(pick, axis=1, keepdims=True), result)
    mass_ref[...] = result


def solution(mesh):
    n_row, n_col = mesh.shape["row"], mesh.shape["col"]

    def shards(pressure, cut_exponent, group_map):
        nx, ny, nz = pressure.shape
        grp = 8
        devices = n_row * n_col
        local = local_matrix(ny)
        wy = np.kron(np.eye(grp), local[:, :ny])
        wu = np.einsum("xw,yk->xykw", np.eye(grp), local[:, ny:]).reshape(grp * ny, 6 * grp)
        eye = np.eye(ny)
        row = lambda i: eye[i]
        near = np.stack(partials_low(row, ny) + partials_high(row))
        ws = np.einsum("ky,xw->kxwy", near, np.eye(grp)).reshape(6 * grp, grp * ny)
        wx = np.kron(np.eye(6), local[:, :ny])
        wc = np.zeros((6, ny, 4, 9))
        for d in range(4):
            for i in range(3):
                for k in range(3):
                    wc[(d // 2) * 3 + i, :, d, 3 * i + k] = local[:, ny + (d % 2) * 3 + k]
        wc = wc.reshape(6 * ny, 36)
        weights = [jnp.asarray(w, BF16) for w in (ws, wy, wu, wx, wc, cyclic_matrix(nz).T)]
        vmem = pl.BlockSpec(memory_space=pltpu.VMEM)
        hbm = pl.BlockSpec(memory_space=pl.ANY)
        return pl.pallas_call(
            functools.partial(kernel, n_row, n_col, grp),
            out_shape=(
                jax.ShapeDtypeStruct((nx, ny, nz), F32),
                jax.ShapeDtypeStruct((GROUPS, len(LEVELS)), F32),
            ),
            in_specs=[hbm] * 9,
            out_specs=(hbm, vmem),
            scratch_shapes=[
                pltpu.VMEM((nx + 8, ny, nz), F32),
                pltpu.VMEM((nx + 6, ny, nz), F32),
                pltpu.VMEM((3, ny, nz), F32),
                pltpu.VMEM((6, nx, nz), F32),
                pltpu.VMEM((6, nx, nz), F32),
                pltpu.VMEM((36, 1, nz), F32),
                pltpu.VMEM((36, 1, nz), F32),
                pltpu.VMEM((1, 128), F32),
                pltpu.VMEM((devices, 1, 128), F32),
                pltpu.VMEM((nx, ny, nz), F32),
                pltpu.SMEM(cut_exponent.shape, jnp.int32),
                pltpu.SMEM(group_map.shape, jnp.int32),
                *(pltpu.VMEM(w.shape, BF16) for w in weights),
                pltpu.SemaphoreType.DMA((3,)),
                pltpu.SemaphoreType.DMA((nx // grp,)),
                pltpu.SemaphoreType.DMA((8,)),
                pltpu.SemaphoreType.DMA((11,)),
                pltpu.SemaphoreType.DMA((11,)),
                pltpu.SemaphoreType.DMA((devices,)),
                pltpu.SemaphoreType.DMA((devices,)),
            ],
            compiler_params=pltpu.CompilerParams(
                collective_id=0, has_side_effects=True, vmem_limit_bytes=62 * 2**20
            ),
        )(cut_exponent, group_map, pressure, *weights)

    specs = P("row", "col", None)
    return jax.shard_map(
        shards, mesh=mesh, in_specs=(specs,) * 3, out_specs=(specs, P()), check_vma=False
    )
```

```python
import functools

import jax
import jax.numpy as jnp
import numpy as np
from jax import lax
from jax.experimental import pallas as pl
from jax.experimental.pallas import tpu as pltpu
from jax.sharding import PartitionSpec as P

GROUPS = 16
LEVELS = (0.25, 0.5, 1.0, 2.0)
MESH = pl.DeviceIdType.MESH
F32, BF16 = jnp.float32, jnp.bfloat16


def cyclic_matrix(n):
    half = n // 2
    ev, od = np.eye(n)[0::2], np.eye(n)[1::2]
    r = lambda a, k: np.roll(a, k, 0)
    d = od - (0.5625 * (ev + r(ev, -1)) - 0.0625 * (r(ev, 1) + r(ev, -2)))
    s = ev + (0.28125 * (r(d, 1) + d) - 0.03125 * (r(d, 2) + r(d, -1)))
    return np.stack([s, d], 1).reshape(n, n) if half else None


def local_matrix(n):
    half = n // 2
    t = np.eye(n + 6)
    v, (a, b, c, f0, f1, g) = t[:n], t[n:]
    e = {j: v[2 * j] for j in range(half)}
    o = {j: v[2 * j + 1] for j in range(half)}
    e[-1], e[half], e[half + 1] = a, f0, f1
    d = {
        j: o[j] - 0.5625 * (e[j] + e[j + 1]) + 0.0625 * (e[j - 1] + e[j + 2])
        for j in range(half)
    }
    d[-1] = b - 0.5625 * e[0] + 0.0625 * e[1]
    d[-2] = c + 0.0625 * e[0]
    d[half] = g + 0.0625 * e[half - 1]
    out = np.zeros((n, n + 6))
    for j in range(half):
        out[2 * j] = e[j] + 0.28125 * (d[j - 1] + d[j]) - 0.03125 * (d[j - 2] + d[j + 1])
        out[2 * j + 1] = d[j]
    return out


def partials_low(row, n):
    a = row(n - 2)
    b = row(n - 1) - 0.5625 * a + 0.0625 * row(n - 4)
    c = row(n - 3) - 0.5625 * (row(n - 4) + a) + 0.0625 * row(n - 6)
    return a, b, c


def partials_high(row):
    f0, f1 = row(0), row(2)
    return f0, f1, row(1) - 0.5625 * (f0 + f1) + 0.0625 * row(4)


def split(value):
    hi = value.astype(BF16)
    return hi, (value - hi.astype(F32)).astype(BF16)


def dot2(left, right):
    dot = functools.partial(jnp.dot, preferred_element_type=F32)
    if left.dtype == BF16:
        hi, lo = split(right)
        return dot(left, hi) + dot(left, lo)
    hi, lo = split(left)
    return dot(hi, right) + dot(lo, right)


def kernel(
    n_row, n_col, grp, cut_hbm, map_hbm, p_ref, *refs
):
    weights, refs = refs[:6], refs[6:]
    out_hbm, mass_ref = refs[:2]
    ext, q, sx, su, u, sc, cb, part, slots, out_ref, cut_ref, map_ref = refs[2:14]
    held = refs[14:20]
    ws_ref, wy_ref, wu_ref, wx_ref, wc_ref, wz_ref = held
    in_sem, o_sem, w_sem, h_send, h_recv, g_send, g_recv = refs[20:]
    nx, ny, nz = p_ref.shape
    devices = n_row * n_col
    row, col = lax.axis_index("row"), lax.axis_index("col")
    me = row * n_col + col
    up_r, dn_r = lax.rem(row + 1, n_row), lax.rem(row + n_row - 1, n_row)
    up_c, dn_c = lax.rem(col + 1, n_col), lax.rem(col + n_col - 1, n_col)

    pieces = ((0, 8), (nx - 8, 8), (8, nx - 16))
    loads = []
    for i, (at, size) in enumerate(pieces):
        load = pltpu.make_async_copy(
            p_ref.at[pl.ds(at, size)], ext.at[pl.ds(at, size)], in_sem.at[i]
        )
        load.start()
        loads.append(load)

    fetched = []
    for i, (src, dst) in enumerate(
        zip((*weights, cut_hbm, map_hbm), (*held, cut_ref, map_ref), strict=True)
    ):
        fetch = pltpu.make_async_copy(src, dst, w_sem.at[i])
        fetch.start()
        fetched.append(fetch)

    def wrap(value, size):
        return lax.select(value >= size, value - size, value)

    def peers(visit):
        @pl.loop(1, n_col)
        def _(k):
            visit(row, wrap(col + k, n_col))

        @pl.loop(1, n_row)
        def _(j):
            other = wrap(row + j, n_row)

            @pl.loop(0, n_col)
            def _(k):
                visit(other, wrap(col + k, n_col))

    barrier = pltpu.get_barrier_semaphore()

    def greet(r, c):
        pl.semaphore_signal(barrier, inc=1, device_id=(r, c), device_id_type=MESH)

    peers(greet)

    sends = []

    def send(src, dst, to):
        i = len(sends)
        copy = pltpu.make_async_remote_copy(
            src_ref=src, dst_ref=dst, send_sem=h_send.at[i], recv_sem=h_recv.at[i],
            device_id=to, device_id_type=MESH,
        )
        copy.start()
        sends.append(copy)

    loads[0].wait()
    loads[1].wait()
    _, b, c = partials_low(lambda i: ext[i], nx)
    sx[0], sx[1] = b, c
    sx[2] = partials_high(lambda i: ext[i])[2]
    loads[2].wait()
    for fetch in fetched:
        fetch.wait()
    for g in range(nx // grp):
        at = pl.ds(g * grp, grp)
        got = dot2(ws_ref[...], ext[at].reshape(grp * ny, nz))
        su[:, at, :] = got.reshape(6, grp, nz)
    for d in range(4):
        for k in range(3):
            plane = (d % 2) * 3 + k
            x_row = lambda i: su[plane, pl.ds(i, 1), :]
            got = partials_low(x_row, nx) if d < 2 else partials_high(x_row)
            for i in range(3):
                sc[9 * d + 3 * i + k] = got[i]

    pl.semaphore_wait(barrier, devices - 1)
    send(sx.at[pl.ds(0, 2)], ext.at[pl.ds(nx + 1, 2)], (up_r, col))
    send(sx.at[2], ext.at[nx + 5], (dn_r, col))
    send(ext.at[nx - 2], ext.at[nx], (up_r, col))
    send(ext.at[0], ext.at[nx + 3], (dn_r, col))
    send(ext.at[2], ext.at[nx + 4], (dn_r, col))
    send(su.at[pl.ds(0, 3)], u.at[pl.ds(0, 3)], (row, up_c))
    send(su.at[pl.ds(3, 3)], u.at[pl.ds(3, 3)], (row, dn_c))
    for d in range(4):
        to = (up_r if d < 2 else dn_r, up_c if d % 2 == 0 else dn_c)
        send(sc.at[pl.ds(9 * d, 9)], cb.at[pl.ds(9 * d, 9)], to)

    for g in range(nx // grp):
        at = pl.ds(g * grp, grp)
        q[at] = dot2(wy_ref[...], ext[at].reshape(grp * ny, nz)).reshape(grp, ny, nz)
    for copy in sends[5:7]:
        copy.wait_recv()
    for g in range(nx // grp):
        at = pl.ds(g * grp, grp)
        more = dot2(wu_ref[...], u[:, at, :].reshape(6 * grp, nz))
        q[at] += more.reshape(grp, ny, nz)
    half = nx // 2

    def x_lift(low, high):
        @pl.loop(0, ny // 8)
        def _(t):
            rows = pl.ds(pl.multiple_of(t * 8, 8), 8)
            far = {-1: nx, half: nx + 3, half + 1: nx + 4}
            first, last = max(low - 3, -1), min(high + 2, half + 1)
            e = {j: q[far.get(j, 2 * j), rows, :] for j in range(first, last + 1)}

            def detail(j):
                if j == -1:
                    return q[nx + 1, rows, :] - 0.5625 * e[0] + 0.0625 * e[1]
                if j == -2:
                    return q[nx + 2, rows, :] + 0.0625 * e[0]
                if j == half:
                    return q[nx + 5, rows, :] + 0.0625 * e[half - 1]
                odd = q[2 * j + 1, rows, :]
                return odd - 0.5625 * (e[j] + e[j + 1]) + 0.0625 * (e[j - 1] + e[j + 2])

            d = {j: detail(j) for j in range(low - 2, low + 1)}
            for j in range(low, high):
                d[j + 1] = detail(j + 1)
                near, wide = d[j - 1] + d[j], d[j - 2] + d[j + 1]
                ext[2 * j, rows, :] = e[j] + 0.28125 * near - 0.03125 * wide
                ext[2 * j + 1, rows, :] = d[j]

    zb = cut_ref.shape[2]
    width = nz // zb
    cuts = jnp.concatenate(
        [jnp.full((1, width), -cut_ref[0, 0, z], jnp.int32) for z in range(zb)], 1
    )
    scale = jnp.exp2(cuts.astype(F32))
    limits = [level * scale for level in LEVELS]
    odd = lambda axis: lax.broadcasted_iota(jnp.int32, (8, nz), axis) % 2
    mixed = (odd(0) + odd(1)) > 0

    def z_group(g, totals):
        at = pl.ds(g * grp, grp)
        made = dot2(ext[at].reshape(grp * ny, nz), wz_ref[...])
        out_ref[at] = made.reshape(grp, ny, nz)
        pltpu.make_async_copy(out_ref.at[at], out_hbm.at[at], o_sem.at[g]).start()
        totals = list(totals)
        for i in range(grp * ny // 8):
            size = jnp.abs(made[8 * i : 8 * i + 8])
            if (8 * i // ny) % 2 == 0:
                size = jnp.where(mixed, size, 0.0)
            for n, limit in enumerate(limits):
                totals[n] += jnp.maximum(size - limit, 0.0)
        return tuple(totals)

    groups = nx // grp
    totals = tuple(jnp.zeros((8, nz), F32) for _ in LEVELS)
    x_lift(grp // 2, half - grp // 2)
    totals = lax.fori_loop(1, groups - 1, z_group, totals)
    for copy in sends[:5] + sends[7:]:
        copy.wait_recv()
    for copy in sends:
        copy.wait_send()
    edge = dot2(wx_ref[...], ext[pl.ds(nx, 6)].reshape(6 * ny, nz))
    edge += dot2(wc_ref[...], cb[...].reshape(-1, nz))
    q[pl.ds(nx, 6)] = edge.reshape(6, ny, nz)
    x_lift(0, grp // 2)
    x_lift(half - grp // 2, half)
    for g in (0, groups - 1):
        totals = z_group(g, totals)
    lane = lax.broadcasted_iota(jnp.int32, (1, 128), 1)
    line = jnp.zeros((1, 128), F32)
    cells = nx * ny * width
    n_lev = len(LEVELS)
    for z in range(zb):
        for n in range(n_lev):
            mass = jnp.sum(totals[n][:, z * width : (z + 1) * width], keepdims=True) / cells
            line += jnp.where(lane == map_ref[0, 0, z] * n_lev + n, mass, 0.0)
    part[...] = line
    slots[me] = line

    def spread(r, c):
        pltpu.make_async_remote_copy(
            src_ref=part, dst_ref=slots.at[me], send_sem=g_send.at[r * n_col + c],
            recv_sem=g_recv.at[me], device_id=(r, c), device_id_type=MESH,
        ).start()

    def gather(r, c):
        t = r * n_col + c
        pltpu.make_async_remote_copy(
            src_ref=part, dst_ref=slots.at[t], send_sem=g_send.at[t],
            recv_sem=g_recv.at[t], device_id=(r, c), device_id_type=MESH,
        ).wait()

    peers(spread)
    peers(gather)
    for g in range(groups):
        at = pl.ds(g * grp, grp)
        pltpu.make_async_copy(out_ref.at[at], out_hbm.at[at], o_sem.at[g]).wait()

    total = jnp.sum(slots[...], axis=0)
    wide = jnp.broadcast_to(total, (GROUPS, 128))
    at_row = lax.broadcasted_iota(jnp.int32, (GROUPS, 128), 0)
    at_lane = lax.broadcasted_iota(jnp.int32, (GROUPS, 128), 1)
    at_col = lax.broadcasted_iota(jnp.int32, (GROUPS, n_lev), 1)
    result = jnp.zeros((GROUPS, n_lev), F32)
    for n in range(n_lev):
        pick = jnp.where(at_lane == at_row * n_lev + n, wide, 0.0)
        result = jnp.where(at_col == n, jnp.sum(pick, axis=1, keepdims=True), result)
    mass_ref[...] = result


def solution(mesh):
    n_row, n_col = mesh.shape["row"], mesh.shape["col"]

    def shards(pressure, cut_exponent, group_map):
        nx, ny, nz = pressure.shape
        grp = 8
        devices = n_row * n_col
        local = local_matrix(ny)
        wy = np.kron(np.eye(grp), local[:, :ny])
        wu = np.einsum("xw,yk->xykw", np.eye(grp), local[:, ny:]).reshape(grp * ny, 6 * grp)
        eye = np.eye(ny)
        row = lambda i: eye[i]
        near = np.stack(partials_low(row, ny) + partials_high(row))
        ws = np.einsum("ky,xw->kxwy", near, np.eye(grp)).reshape(6 * grp, grp * ny)
        wx = np.kron(np.eye(6), local[:, :ny])
        wc = np.zeros((6, ny, 4, 9))
        for d in range(4):
            for i in range(3):
                for k in range(3):
                    wc[(d // 2) * 3 + i, :, d, 3 * i + k] = local[:, ny + (d % 2) * 3 + k]
        wc = wc.reshape(6 * ny, 36)
        weights = [jnp.asarray(w, BF16) for w in (ws, wy, wu, wx, wc, cyclic_matrix(nz).T)]
        vmem = pl.BlockSpec(memory_space=pltpu.VMEM)
        hbm = pl.BlockSpec(memory_space=pl.ANY)
        return pl.pallas_call(
            functools.partial(kernel, n_row, n_col, grp),
            out_shape=(
                jax.ShapeDtypeStruct((nx, ny, nz), F32),
                jax.ShapeDtypeStruct((GROUPS, len(LEVELS)), F32),
            ),
            in_specs=[hbm] * 9,
            out_specs=(hbm, vmem),
            scratch_shapes=[
                pltpu.VMEM((nx + 8, ny, nz), F32),
                pltpu.VMEM((nx + 6, ny, nz), F32),
                pltpu.VMEM((3, ny, nz), F32),
                pltpu.VMEM((6, nx, nz), F32),
                pltpu.VMEM((6, nx, nz), F32),
                pltpu.VMEM((36, 1, nz), F32),
                pltpu.VMEM((36, 1, nz), F32),
                pltpu.VMEM((1, 128), F32),
                pltpu.VMEM((devices, 1, 128), F32),
                pltpu.VMEM((nx, ny, nz), F32),
                pltpu.SMEM(cut_exponent.shape, jnp.int32),
                pltpu.SMEM(group_map.shape, jnp.int32),
                *(pltpu.VMEM(w.shape, BF16) for w in weights),
                pltpu.SemaphoreType.DMA((3,)),
                pltpu.SemaphoreType.DMA((nx // grp,)),
                pltpu.SemaphoreType.DMA((8,)),
                pltpu.SemaphoreType.DMA((11,)),
                pltpu.SemaphoreType.DMA((11,)),
                pltpu.SemaphoreType.DMA((devices,)),
                pltpu.SemaphoreType.DMA((devices,)),
            ],
            compiler_params=pltpu.CompilerParams(
                collective_id=0, has_side_effects=True, vmem_limit_bytes=62 * 2**20
            ),
        )(cut_exponent, group_map, pressure, *weights)

    specs = P("row", "col", None)
    return jax.shard_map(
        shards, mesh=mesh, in_specs=(specs,) * 3, out_specs=(specs, P()), check_vma=False
    )
```

```python
import functools

import jax
import jax.numpy as jnp
import numpy as np
from jax import lax
from jax.experimental import pallas as pl
from jax.experimental.pallas import tpu as pltpu
from jax.sharding import PartitionSpec as P

GROUPS = 16
LEVELS = (0.25, 0.5, 1.0, 2.0)
MESH = pl.DeviceIdType.MESH
F32, BF16 = jnp.float32, jnp.bfloat16


def cyclic_matrix(n):
    half = n // 2
    ev, od = np.eye(n)[0::2], np.eye(n)[1::2]
    r = lambda a, k: np.roll(a, k, 0)
    d = od - (0.5625 * (ev + r(ev, -1)) - 0.0625 * (r(ev, 1) + r(ev, -2)))
    s = ev + (0.28125 * (r(d, 1) + d) - 0.03125 * (r(d, 2) + r(d, -1)))
    return np.stack([s, d], 1).reshape(n, n) if half else None


def local_matrix(n):
    half = n // 2
    t = np.eye(n + 6)
    v, (a, b, c, f0, f1, g) = t[:n], t[n:]
    e = {j: v[2 * j] for j in range(half)}
    o = {j: v[2 * j + 1] for j in range(half)}
    e[-1], e[half], e[half + 1] = a, f0, f1
    d = {
        j: o[j] - 0.5625 * (e[j] + e[j + 1]) + 0.0625 * (e[j - 1] + e[j + 2])
        for j in range(half)
    }
    d[-1] = b - 0.5625 * e[0] + 0.0625 * e[1]
    d[-2] = c + 0.0625 * e[0]
    d[half] = g + 0.0625 * e[half - 1]
    out = np.zeros((n, n + 6))
    for j in range(half):
        out[2 * j] = e[j] + 0.28125 * (d[j - 1] + d[j]) - 0.03125 * (d[j - 2] + d[j + 1])
        out[2 * j + 1] = d[j]
    return out


def partials_low(row, n):
    a = row(n - 2)
    b = row(n - 1) - 0.5625 * a + 0.0625 * row(n - 4)
    c = row(n - 3) - 0.5625 * (row(n - 4) + a) + 0.0625 * row(n - 6)
    return a, b, c


def partials_high(row):
    f0, f1 = row(0), row(2)
    return f0, f1, row(1) - 0.5625 * (f0 + f1) + 0.0625 * row(4)


def split(value):
    hi = value.astype(BF16)
    return hi, (value - hi.astype(F32)).astype(BF16)


def dot2(left, right):
    dot = functools.partial(jnp.dot, preferred_element_type=F32)
    if left.dtype == BF16:
        hi, lo = split(right)
        return dot(left, hi) + dot(left, lo)
    hi, lo = split(left)
    return dot(hi, right) + dot(lo, right)


def kernel(
    n_row, n_col, grp, cut_hbm, map_hbm, p_ref, *refs
):
    weights, refs = refs[:6], refs[6:]
    out_hbm, mass_ref = refs[:2]
    ext, q, sx, su, u, sc, cb, part, slots, out_ref, cut_ref, map_ref = refs[2:14]
    held = refs[14:20]
    ws_ref, wy_ref, wu_ref, wx_ref, wc_ref, wz_ref = held
    in_sem, o_sem, w_sem, h_send, h_recv, g_send, g_recv = refs[20:]
    nx, ny, nz = p_ref.shape
    devices = n_row * n_col
    row, col = lax.axis_index("row"), lax.axis_index("col")
    me = row * n_col + col
    up_r, dn_r = lax.rem(row + 1, n_row), lax.rem(row + n_row - 1, n_row)
    up_c, dn_c = lax.rem(col + 1, n_col), lax.rem(col + n_col - 1, n_col)

    pieces = ((0, 8), (nx - 8, 8), (8, nx - 16))
    loads = []
    for i, (at, size) in enumerate(pieces):
        load = pltpu.make_async_copy(
            p_ref.at[pl.ds(at, size)], ext.at[pl.ds(at, size)], in_sem.at[i]
        )
        load.start()
        loads.append(load)

    fetched = []
    for i, (src, dst) in enumerate(
        zip((*weights, cut_hbm, map_hbm), (*held, cut_ref, map_ref), strict=True)
    ):
        fetch = pltpu.make_async_copy(src, dst, w_sem.at[i])
        fetch.start()
        fetched.append(fetch)

    def wrap(value, size):
        return lax.select(value >= size, value - size, value)

    def peers(visit):
        @pl.loop(1, n_col)
        def _(k):
            visit(row, wrap(col + k, n_col))

        @pl.loop(1, n_row)
        def _(j):
            other = wrap(row + j, n_row)

            @pl.loop(0, n_col)
            def _(k):
                visit(other, wrap(col + k, n_col))

    barrier = pltpu.get_barrier_semaphore()

    def greet(r, c):
        pl.semaphore_signal(barrier, inc=1, device_id=(r, c), device_id_type=MESH)

    peers(greet)

    sends = []

    def send(src, dst, to):
        i = len(sends)
        copy = pltpu.make_async_remote_copy(
            src_ref=src, dst_ref=dst, send_sem=h_send.at[i], recv_sem=h_recv.at[i],
            device_id=to, device_id_type=MESH,
        )
        copy.start()
        sends.append(copy)

    loads[0].wait()
    loads[1].wait()
    _, b, c = partials_low(lambda i: ext[i], nx)
    sx[0], sx[1] = b, c
    sx[2] = partials_high(lambda i: ext[i])[2]
    loads[2].wait()
    for fetch in fetched:
        fetch.wait()
    for g in range(nx // grp):
        at = pl.ds(g * grp, grp)
        got = dot2(ws_ref[...], ext[at].reshape(grp * ny, nz))
        su[:, at, :] = got.reshape(6, grp, nz)
    for d in range(4):
        for k in range(3):
            plane = (d % 2) * 3 + k
            x_row = lambda i: su[plane, pl.ds(i, 1), :]
            got = partials_low(x_row, nx) if d < 2 else partials_high(x_row)
            for i in range(3):
                sc[9 * d + 3 * i + k] = got[i]

    pl.semaphore_wait(barrier, devices - 1)
    send(sx.at[pl.ds(0, 2)], ext.at[pl.ds(nx + 1, 2)], (up_r, col))
    send(sx.at[2], ext.at[nx + 5], (dn_r, col))
    send(ext.at[nx - 2], ext.at[nx], (up_r, col))
    send(ext.at[0], ext.at[nx + 3], (dn_r, col))
    send(ext.at[2], ext.at[nx + 4], (dn_r, col))
    send(su.at[pl.ds(0, 3)], u.at[pl.ds(0, 3)], (row, up_c))
    send(su.at[pl.ds(3, 3)], u.at[pl.ds(3, 3)], (row, dn_c))
    for d in range(4):
        to = (up_r if d < 2 else dn_r, up_c if d % 2 == 0 else dn_c)
        send(sc.at[pl.ds(9 * d, 9)], cb.at[pl.ds(9 * d, 9)], to)

    for g in range(nx // grp):
        at = pl.ds(g * grp, grp)
        q[at] = dot2(wy_ref[...], ext[at].reshape(grp * ny, nz)).reshape(grp, ny, nz)
    for copy in sends[5:7]:
        copy.wait_recv()
    for g in range(nx // grp):
        at = pl.ds(g * grp, grp)
        more = dot2(wu_ref[...], u[:, at, :].reshape(6 * grp, nz))
        q[at] += more.reshape(grp, ny, nz)
    half = nx // 2

    def x_lift(low, high):
        @pl.loop(0, ny // 8)
        def _(t):
            rows = pl.ds(pl.multiple_of(t * 8, 8), 8)
            far = {-1: nx, half: nx + 3, half + 1: nx + 4}
            first, last = max(low - 3, -1), min(high + 2, half + 1)
            e = {j: q[far.get(j, 2 * j), rows, :] for j in range(first, last + 1)}

            def detail(j):
                if j == -1:
                    return q[nx + 1, rows, :] - 0.5625 * e[0] + 0.0625 * e[1]
                if j == -2:
                    return q[nx + 2, rows, :] + 0.0625 * e[0]
                if j == half:
                    return q[nx + 5, rows, :] + 0.0625 * e[half - 1]
                odd = q[2 * j + 1, rows, :]
                return odd - 0.5625 * (e[j] + e[j + 1]) + 0.0625 * (e[j - 1] + e[j + 2])

            d = {j: detail(j) for j in range(low - 2, low + 1)}
            for j in range(low, high):
                d[j + 1] = detail(j + 1)
                near, wide = d[j - 1] + d[j], d[j - 2] + d[j + 1]
                ext[2 * j, rows, :] = e[j] + 0.28125 * near - 0.03125 * wide
                ext[2 * j + 1, rows, :] = d[j]

    zb = cut_ref.shape[2]
    width = nz // zb
    cuts = jnp.concatenate(
        [jnp.full((1, width), -cut_ref[0, 0, z], jnp.int32) for z in range(zb)], 1
    )
    scale = jnp.exp2(cuts.astype(F32))
    limits = [level * scale for level in LEVELS]
    odd = lambda axis: lax.broadcasted_iota(jnp.int32, (8, nz), axis) % 2
    mixed = (odd(0) + odd(1)) > 0

    def z_group(g, totals):
        at = pl.ds(g * grp, grp)
        made = dot2(ext[at].reshape(grp * ny, nz), wz_ref[...])
        out_ref[at] = made.reshape(grp, ny, nz)
        pltpu.make_async_copy(out_ref.at[at], out_hbm.at[at], o_sem.at[g]).start()
        totals = list(totals)
        for i in range(grp * ny // 8):
            size = jnp.abs(made[8 * i : 8 * i + 8])
            if (8 * i // ny) % 2 == 0:
                size = jnp.where(mixed, size, 0.0)
            for n, limit in enumerate(limits):
                totals[n] += jnp.maximum(size - limit, 0.0)
        return tuple(totals)

    groups = nx // grp
    totals = tuple(jnp.zeros((8, nz), F32) for _ in LEVELS)
    x_lift(grp // 2, half - grp // 2)
    totals = lax.fori_loop(1, groups - 1, z_group, totals)
    for copy in sends[:5] + sends[7:]:
        copy.wait_recv()
    for copy in sends:
        copy.wait_send()
    edge = dot2(wx_ref[...], ext[pl.ds(nx, 6)].reshape(6 * ny, nz))
    edge += dot2(wc_ref[...], cb[...].reshape(-1, nz))
    q[pl.ds(nx, 6)] = edge.reshape(6, ny, nz)
    x_lift(0, grp // 2)
    x_lift(half - grp // 2, half)
    for g in (0, groups - 1):
        totals = z_group(g, totals)
    lane = lax.broadcasted_iota(jnp.int32, (1, 128), 1)
    line = jnp.zeros((1, 128), F32)
    cells = nx * ny * width
    n_lev = len(LEVELS)
    for z in range(zb):
        for n in range(n_lev):
            mass = jnp.sum(totals[n][:, z * width : (z + 1) * width], keepdims=True) / cells
            line += jnp.where(lane == n * GROUPS + map_ref[0, 0, z], mass, 0.0)
    part[...] = line
    slots[me] = line

    def spread(r, c):
        pltpu.make_async_remote_copy(
            src_ref=part, dst_ref=slots.at[me], send_sem=g_send.at[r * n_col + c],
            recv_sem=g_recv.at[me], device_id=(r, c), device_id_type=MESH,
        ).start()

    def gather(r, c):
        t = r * n_col + c
        pltpu.make_async_remote_copy(
            src_ref=part, dst_ref=slots.at[t], send_sem=g_send.at[t],
            recv_sem=g_recv.at[t], device_id=(r, c), device_id_type=MESH,
        ).wait()

    peers(spread)
    peers(gather)
    for g in range(groups):
        at = pl.ds(g * grp, grp)
        pltpu.make_async_copy(out_ref.at[at], out_hbm.at[at], o_sem.at[g]).wait()

    total = jnp.sum(slots[...], axis=0)
    mass_ref[...] = jnp.concatenate(
        [total[:, n * GROUPS : (n + 1) * GROUPS] for n in range(n_lev)], 0
    )


def deliver(c_hbm, m_hbm, out_hbm, mass_hbm, held, line, sems, m_sems):
    count = sems.shape[1]
    size = held.shape[0] // count
    piece = [pl.ds(i * size, size) for i in range(count)]
    copy = pltpu.make_async_copy
    ins = [copy(c_hbm.at[p], held.at[p], sems.at[0, i]) for i, p in enumerate(piece)]
    outs = [copy(held.at[p], out_hbm.at[p], sems.at[1, i]) for i, p in enumerate(piece)]
    ins.insert(1, copy(m_hbm, line, m_sems.at[0]))
    outs.insert(1, copy(line, mass_hbm, m_sems.at[1]))
    for c in ins:
        c.start()
    for c, o in zip(ins, outs, strict=True):
        c.wait()
        o.start()
    for o in outs:
        o.wait()


def solution(mesh):
    n_row, n_col = mesh.shape["row"], mesh.shape["col"]

    def shards(pressure, cut_exponent, group_map):
        nx, ny, nz = pressure.shape
        grp = 8
        devices = n_row * n_col
        local = local_matrix(ny)
        wy = np.kron(np.eye(grp), local[:, :ny])
        wu = np.einsum("xw,yk->xykw", np.eye(grp), local[:, ny:]).reshape(grp * ny, 6 * grp)
        eye = np.eye(ny)
        row = lambda i: eye[i]
        near = np.stack(partials_low(row, ny) + partials_high(row))
        ws = np.einsum("ky,xw->kxwy", near, np.eye(grp)).reshape(6 * grp, grp * ny)
        wx = np.kron(np.eye(6), local[:, :ny])
        wc = np.zeros((6, ny, 4, 9))
        for d in range(4):
            for i in range(3):
                for k in range(3):
                    wc[(d // 2) * 3 + i, :, d, 3 * i + k] = local[:, ny + (d % 2) * 3 + k]
        wc = wc.reshape(6 * ny, 36)
        weights = [jnp.asarray(w, BF16) for w in (ws, wy, wu, wx, wc, cyclic_matrix(nz).T)]
        vmem = pl.BlockSpec(memory_space=pltpu.VMEM)
        hbm = pl.BlockSpec(memory_space=pl.ANY)
        found = pl.pallas_call(
            functools.partial(kernel, n_row, n_col, grp),
            out_shape=(
                jax.ShapeDtypeStruct((nx, ny, nz), F32),
                jax.ShapeDtypeStruct((len(LEVELS), GROUPS), F32),
            ),
            in_specs=[hbm] * 9,
            out_specs=(hbm, vmem),
            scratch_shapes=[
                pltpu.VMEM((nx + 8, ny, nz), F32),
                pltpu.VMEM((nx + 6, ny, nz), F32),
                pltpu.VMEM((3, ny, nz), F32),
                pltpu.VMEM((6, nx, nz), F32),
                pltpu.VMEM((6, nx, nz), F32),
                pltpu.VMEM((36, 1, nz), F32),
                pltpu.VMEM((36, 1, nz), F32),
                pltpu.VMEM((1, 128), F32),
                pltpu.VMEM((devices, 1, 128), F32),
                pltpu.VMEM((nx, ny, nz), F32),
                pltpu.SMEM(cut_exponent.shape, jnp.int32),
                pltpu.SMEM(group_map.shape, jnp.int32),
                *(pltpu.VMEM(w.shape, BF16) for w in weights),
                pltpu.SemaphoreType.DMA((3,)),
                pltpu.SemaphoreType.DMA((nx // grp,)),
                pltpu.SemaphoreType.DMA((8,)),
                pltpu.SemaphoreType.DMA((11,)),
                pltpu.SemaphoreType.DMA((11,)),
                pltpu.SemaphoreType.DMA((devices,)),
                pltpu.SemaphoreType.DMA((devices,)),
            ],
            compiler_params=pltpu.CompilerParams(
                collective_id=0, has_side_effects=True, vmem_limit_bytes=62 * 2**20
            ),
        )(cut_exponent, group_map, pressure, *weights)
        coeffs, mass = pl.pallas_call(
            deliver,
            out_shape=tuple(jax.ShapeDtypeStruct(f.shape, F32) for f in found),
            in_specs=[hbm] * 2,
            out_specs=(hbm, hbm),
            scratch_shapes=[
                pltpu.VMEM((nx, ny, nz), F32),
                pltpu.VMEM(found[1].shape, F32),
                pltpu.SemaphoreType.DMA((2, 8)),
                pltpu.SemaphoreType.DMA((2,)),
            ],
            compiler_params=pltpu.CompilerParams(vmem_limit_bytes=62 * 2**20),
        )(*found)
        return coeffs, mass.T

    specs = P("row", "col", None)
    return jax.shard_map(
        shards, mesh=mesh, in_specs=(specs,) * 3, out_specs=(specs, P()), check_vma=False
    )
```

```python
import functools

import jax
import jax.numpy as jnp
import numpy as np
from jax import lax
from jax.experimental import pallas as pl
from jax.experimental.pallas import tpu as pltpu
from jax.sharding import PartitionSpec as P

GROUPS = 16
LEVELS = (0.25, 0.5, 1.0, 2.0)
MESH = pl.DeviceIdType.MESH
F32, BF16 = jnp.float32, jnp.bfloat16


def cyclic_matrix(n):
    half = n // 2
    ev, od = np.eye(n)[0::2], np.eye(n)[1::2]
    r = lambda a, k: np.roll(a, k, 0)
    d = od - (0.5625 * (ev + r(ev, -1)) - 0.0625 * (r(ev, 1) + r(ev, -2)))
    s = ev + (0.28125 * (r(d, 1) + d) - 0.03125 * (r(d, 2) + r(d, -1)))
    return np.stack([s, d], 1).reshape(n, n) if half else None


def local_matrix(n):
    half = n // 2
    t = np.eye(n + 6)
    v, (a, b, c, f0, f1, g) = t[:n], t[n:]
    e = {j: v[2 * j] for j in range(half)}
    o = {j: v[2 * j + 1] for j in range(half)}
    e[-1], e[half], e[half + 1] = a, f0, f1
    d = {
        j: o[j] - 0.5625 * (e[j] + e[j + 1]) + 0.0625 * (e[j - 1] + e[j + 2])
        for j in range(half)
    }
    d[-1] = b - 0.5625 * e[0] + 0.0625 * e[1]
    d[-2] = c + 0.0625 * e[0]
    d[half] = g + 0.0625 * e[half - 1]
    out = np.zeros((n, n + 6))
    for j in range(half):
        out[2 * j] = e[j] + 0.28125 * (d[j - 1] + d[j]) - 0.03125 * (d[j - 2] + d[j + 1])
        out[2 * j + 1] = d[j]
    return out


def partials_low(row, n):
    a = row(n - 2)
    b = row(n - 1) - 0.5625 * a + 0.0625 * row(n - 4)
    c = row(n - 3) - 0.5625 * (row(n - 4) + a) + 0.0625 * row(n - 6)
    return a, b, c


def partials_high(row):
    f0, f1 = row(0), row(2)
    return f0, f1, row(1) - 0.5625 * (f0 + f1) + 0.0625 * row(4)


def split(value):
    hi = value.astype(BF16)
    return hi, (value - hi.astype(F32)).astype(BF16)


def dot2(left, right):
    dot = functools.partial(jnp.dot, preferred_element_type=F32)
    if left.dtype == BF16:
        hi, lo = split(right)
        return dot(left, hi) + dot(left, lo)
    hi, lo = split(left)
    return dot(hi, right) + dot(lo, right)


def kernel(
    n_row, n_col, grp, cut_hbm, map_hbm, p_ref, *refs
):
    weights, refs = refs[:6], refs[6:]
    out_hbm, mass_ref = refs[:2]
    ext, q, sx, su, u, sc, cb, part, slots, out_ref, cut_ref, map_ref = refs[2:14]
    held = refs[14:20]
    ws_ref, wy_ref, wu_ref, wx_ref, wc_ref, wz_ref = held
    in_sem, o_sem, w_sem, h_send, h_recv, g_send, g_recv, hop_sem = refs[20:]
    nx, ny, nz = p_ref.shape
    devices = n_row * n_col
    row, col = lax.axis_index("row"), lax.axis_index("col")
    me = row * n_col + col
    up_r, dn_r = lax.rem(row + 1, n_row), lax.rem(row + n_row - 1, n_row)
    up_c, dn_c = lax.rem(col + 1, n_col), lax.rem(col + n_col - 1, n_col)

    pieces = ((0, 8), (nx - 8, 8), (8, nx - 16))
    loads = []
    for i, (at, size) in enumerate(pieces):
        load = pltpu.make_async_copy(
            p_ref.at[pl.ds(at, size)], ext.at[pl.ds(at, size)], in_sem.at[i]
        )
        load.start()
        loads.append(load)

    fetched = []
    for i, (src, dst) in enumerate(
        zip((*weights, cut_hbm, map_hbm), (*held, cut_ref, map_ref), strict=True)
    ):
        fetch = pltpu.make_async_copy(src, dst, w_sem.at[i])
        fetch.start()
        fetched.append(fetch)

    def wrap(value, size):
        return lax.select(value >= size, value - size, value)

    def peers(visit):
        @pl.loop(1, n_col)
        def _(k):
            visit(row, wrap(col + k, n_col))

        @pl.loop(1, n_row)
        def _(j):
            other = wrap(row + j, n_row)

            @pl.loop(0, n_col)
            def _(k):
                visit(other, wrap(col + k, n_col))

    barrier = pltpu.get_barrier_semaphore()

    def greet(r, c):
        pl.semaphore_signal(barrier, inc=1, device_id=(r, c), device_id_type=MESH)

    for r, c in ((up_r, col), (dn_r, col), (row, up_c), (row, dn_c)):
        greet(r, c)
    along_col = max(n_col // 2 - 1, 1)
    hops = along_col + n_row // 2

    def call(k):
        aim = ((row, up_c), (row, dn_c)) if k < along_col else ((up_r, col), (dn_r, col))
        for to in aim:
            pl.semaphore_signal(hop_sem.at[k], inc=1, device_id=to, device_id_type=MESH)

    def relay(k):
        pl.semaphore_wait(hop_sem.at[k], 2)
        if k + 1 < hops:
            call(k + 1)


    sends = []

    def send(src, dst, to):
        i = len(sends)
        copy = pltpu.make_async_remote_copy(
            src_ref=src, dst_ref=dst, send_sem=h_send.at[i], recv_sem=h_recv.at[i],
            device_id=to, device_id_type=MESH,
        )
        copy.start()
        sends.append(copy)

    loads[0].wait()
    loads[1].wait()
    _, b, c = partials_low(lambda i: ext[i], nx)
    sx[0], sx[1] = b, c
    sx[2] = partials_high(lambda i: ext[i])[2]
    loads[2].wait()
    for fetch in fetched:
        fetch.wait()
    for g in range(nx // grp):
        at = pl.ds(g * grp, grp)
        got = dot2(ws_ref[...], ext[at].reshape(grp * ny, nz))
        su[:, at, :] = got.reshape(6, grp, nz)
    for d in range(4):
        for k in range(3):
            plane = (d % 2) * 3 + k
            x_row = lambda i: su[plane, pl.ds(i, 1), :]
            got = partials_low(x_row, nx) if d < 2 else partials_high(x_row)
            for i in range(3):
                sc[9 * d + 3 * i + k] = got[i]

    pl.semaphore_wait(barrier, 4)
    call(0)
    send(sx.at[pl.ds(0, 2)], ext.at[pl.ds(nx + 1, 2)], (up_r, col))
    send(sx.at[2], ext.at[nx + 5], (dn_r, col))
    send(ext.at[nx - 2], ext.at[nx], (up_r, col))
    send(ext.at[0], ext.at[nx + 3], (dn_r, col))
    send(ext.at[2], ext.at[nx + 4], (dn_r, col))
    send(su.at[pl.ds(0, 3)], u.at[pl.ds(0, 3)], (row, up_c))
    send(su.at[pl.ds(3, 3)], u.at[pl.ds(3, 3)], (row, dn_c))
    relay(0)
    for d in range(4):
        to = (up_r if d < 2 else dn_r, up_c if d % 2 == 0 else dn_c)
        send(sc.at[pl.ds(9 * d, 9)], cb.at[pl.ds(9 * d, 9)], to)

    for g in range(nx // grp):
        at = pl.ds(g * grp, grp)
        q[at] = dot2(wy_ref[...], ext[at].reshape(grp * ny, nz)).reshape(grp, ny, nz)
    relay(1)
    for copy in sends[5:7]:
        copy.wait_recv()
    relay(2)
    for g in range(nx // grp):
        at = pl.ds(g * grp, grp)
        more = dot2(wu_ref[...], u[:, at, :].reshape(6 * grp, nz))
        q[at] += more.reshape(grp, ny, nz)
    half = nx // 2
    relay(3)

    def x_lift(low, high):
        @pl.loop(0, ny // 8)
        def _(t):
            rows = pl.ds(pl.multiple_of(t * 8, 8), 8)
            far = {-1: nx, half: nx + 3, half + 1: nx + 4}
            first, last = max(low - 3, -1), min(high + 2, half + 1)
            e = {j: q[far.get(j, 2 * j), rows, :] for j in range(first, last + 1)}

            def detail(j):
                if j == -1:
                    return q[nx + 1, rows, :] - 0.5625 * e[0] + 0.0625 * e[1]
                if j == -2:
                    return q[nx + 2, rows, :] + 0.0625 * e[0]
                if j == half:
                    return q[nx + 5, rows, :] + 0.0625 * e[half - 1]
                odd = q[2 * j + 1, rows, :]
                return odd - 0.5625 * (e[j] + e[j + 1]) + 0.0625 * (e[j - 1] + e[j + 2])

            d = {j: detail(j) for j in range(low - 2, low + 1)}
            for j in range(low, high):
                d[j + 1] = detail(j + 1)
                near, wide = d[j - 1] + d[j], d[j - 2] + d[j + 1]
                ext[2 * j, rows, :] = e[j] + 0.28125 * near - 0.03125 * wide
                ext[2 * j + 1, rows, :] = d[j]

    zb = cut_ref.shape[2]
    width = nz // zb
    cuts = jnp.concatenate(
        [jnp.full((1, width), -cut_ref[0, 0, z], jnp.int32) for z in range(zb)], 1
    )
    scale = jnp.exp2(cuts.astype(F32))
    limits = [level * scale for level in LEVELS]
    odd = lambda axis: lax.broadcasted_iota(jnp.int32, (8, nz), axis) % 2
    mixed = (odd(0) + odd(1)) > 0

    def z_group(g, totals):
        at = pl.ds(g * grp, grp)
        made = dot2(ext[at].reshape(grp * ny, nz), wz_ref[...])
        out_ref[at] = made.reshape(grp, ny, nz)
        pltpu.make_async_copy(out_ref.at[at], out_hbm.at[at], o_sem.at[g]).start()
        totals = list(totals)
        for i in range(grp * ny // 8):
            size = jnp.abs(made[8 * i : 8 * i + 8])
            if (8 * i // ny) % 2 == 0:
                size = jnp.where(mixed, size, 0.0)
            for n, limit in enumerate(limits):
                totals[n] += jnp.maximum(size - limit, 0.0)
        return tuple(totals)

    groups = nx // grp
    totals = tuple(jnp.zeros((8, nz), F32) for _ in LEVELS)
    x_lift(grp // 2, half - grp // 2)
    totals = lax.fori_loop(1, groups - 1, z_group, totals)
    for k in range(4, hops):
        relay(k)
    for copy in sends[:5] + sends[7:]:
        copy.wait_recv()
    for copy in sends:
        copy.wait_send()
    edge = dot2(wx_ref[...], ext[pl.ds(nx, 6)].reshape(6 * ny, nz))
    edge += dot2(wc_ref[...], cb[...].reshape(-1, nz))
    q[pl.ds(nx, 6)] = edge.reshape(6, ny, nz)
    x_lift(0, grp // 2)
    x_lift(half - grp // 2, half)
    for g in (0, groups - 1):
        totals = z_group(g, totals)
    lane = lax.broadcasted_iota(jnp.int32, (1, 128), 1)
    line = jnp.zeros((1, 128), F32)
    cells = nx * ny * width
    n_lev = len(LEVELS)
    for z in range(zb):
        for n in range(n_lev):
            mass = jnp.sum(totals[n][:, z * width : (z + 1) * width], keepdims=True) / cells
            line += jnp.where(lane == n * GROUPS + map_ref[0, 0, z], mass, 0.0)
    part[...] = line
    slots[me] = line

    def spread(r, c):
        pltpu.make_async_remote_copy(
            src_ref=part, dst_ref=slots.at[me], send_sem=g_send.at[r * n_col + c],
            recv_sem=g_recv.at[me], device_id=(r, c), device_id_type=MESH,
        ).start()

    def gather(r, c):
        t = r * n_col + c
        pltpu.make_async_remote_copy(
            src_ref=part, dst_ref=slots.at[t], send_sem=g_send.at[t],
            recv_sem=g_recv.at[t], device_id=(r, c), device_id_type=MESH,
        ).wait()

    peers(spread)
    peers(gather)
    for g in range(groups):
        at = pl.ds(g * grp, grp)
        pltpu.make_async_copy(out_ref.at[at], out_hbm.at[at], o_sem.at[g]).wait()

    total = jnp.sum(slots[...], axis=0)
    mass_ref[...] = jnp.concatenate(
        [total[:, n * GROUPS : (n + 1) * GROUPS] for n in range(n_lev)], 0
    )


def deliver(c_hbm, m_hbm, out_hbm, mass_hbm, held, line, sems, m_sems):
    count = sems.shape[1]
    size = held.shape[0] // count
    piece = [pl.ds(i * size, size) for i in range(count)]
    copy = pltpu.make_async_copy
    ins = [copy(c_hbm.at[p], held.at[p], sems.at[0, i]) for i, p in enumerate(piece)]
    outs = [copy(held.at[p], out_hbm.at[p], sems.at[1, i]) for i, p in enumerate(piece)]
    ins.insert(1, copy(m_hbm, line, m_sems.at[0]))
    outs.insert(1, copy(line, mass_hbm, m_sems.at[1]))
    for c in ins:
        c.start()
    for c, o in zip(ins, outs, strict=True):
        c.wait()
        o.start()
    for o in outs:
        o.wait()


def solution(mesh):
    n_row, n_col = mesh.shape["row"], mesh.shape["col"]

    def shards(pressure, cut_exponent, group_map):
        nx, ny, nz = pressure.shape
        grp = 8
        devices = n_row * n_col
        local = local_matrix(ny)
        wy = np.kron(np.eye(grp), local[:, :ny])
        wu = np.einsum("xw,yk->xykw", np.eye(grp), local[:, ny:]).reshape(grp * ny, 6 * grp)
        eye = np.eye(ny)
        row = lambda i: eye[i]
        near = np.stack(partials_low(row, ny) + partials_high(row))
        ws = np.einsum("ky,xw->kxwy", near, np.eye(grp)).reshape(6 * grp, grp * ny)
        wx = np.kron(np.eye(6), local[:, :ny])
        wc = np.zeros((6, ny, 4, 9))
        for d in range(4):
            for i in range(3):
                for k in range(3):
                    wc[(d // 2) * 3 + i, :, d, 3 * i + k] = local[:, ny + (d % 2) * 3 + k]
        wc = wc.reshape(6 * ny, 36)
        weights = [jnp.asarray(w, BF16) for w in (ws, wy, wu, wx, wc, cyclic_matrix(nz).T)]
        vmem = pl.BlockSpec(memory_space=pltpu.VMEM)
        hbm = pl.BlockSpec(memory_space=pl.ANY)
        found = pl.pallas_call(
            functools.partial(kernel, n_row, n_col, grp),
            out_shape=(
                jax.ShapeDtypeStruct((nx, ny, nz), F32),
                jax.ShapeDtypeStruct((len(LEVELS), GROUPS), F32),
            ),
            in_specs=[hbm] * 9,
            out_specs=(hbm, vmem),
            scratch_shapes=[
                pltpu.VMEM((nx + 8, ny, nz), F32),
                pltpu.VMEM((nx + 6, ny, nz), F32),
                pltpu.VMEM((3, ny, nz), F32),
                pltpu.VMEM((6, nx, nz), F32),
                pltpu.VMEM((6, nx, nz), F32),
                pltpu.VMEM((36, 1, nz), F32),
                pltpu.VMEM((36, 1, nz), F32),
                pltpu.VMEM((1, 128), F32),
                pltpu.VMEM((devices, 1, 128), F32),
                pltpu.VMEM((nx, ny, nz), F32),
                pltpu.SMEM(cut_exponent.shape, jnp.int32),
                pltpu.SMEM(group_map.shape, jnp.int32),
                *(pltpu.VMEM(w.shape, BF16) for w in weights),
                pltpu.SemaphoreType.DMA((3,)),
                pltpu.SemaphoreType.DMA((nx // grp,)),
                pltpu.SemaphoreType.DMA((8,)),
                pltpu.SemaphoreType.DMA((11,)),
                pltpu.SemaphoreType.DMA((11,)),
                pltpu.SemaphoreType.DMA((devices,)),
                pltpu.SemaphoreType.DMA((devices,)),
                pltpu.SemaphoreType.REGULAR((n_col // 2 + n_row // 2,)),
            ],
            compiler_params=pltpu.CompilerParams(
                collective_id=0, has_side_effects=True, vmem_limit_bytes=62 * 2**20
            ),
        )(cut_exponent, group_map, pressure, *weights)
        coeffs, mass = pl.pallas_call(
            deliver,
            out_shape=tuple(jax.ShapeDtypeStruct(f.shape, F32) for f in found),
            in_specs=[hbm] * 2,
            out_specs=(hbm, hbm),
            scratch_shapes=[
                pltpu.VMEM((nx, ny, nz), F32),
                pltpu.VMEM(found[1].shape, F32),
                pltpu.SemaphoreType.DMA((2, 8)),
                pltpu.SemaphoreType.DMA((2,)),
            ],
            compiler_params=pltpu.CompilerParams(vmem_limit_bytes=62 * 2**20),
        )(*found)
        return coeffs, mass.T

    specs = P("row", "col", None)
    return jax.shard_map(
        shards, mesh=mesh, in_specs=(specs,) * 3, out_specs=(specs, P()), check_vma=False
    )
```

```python
import functools

import jax
import jax.numpy as jnp
import numpy as np
from jax import lax
from jax.experimental import pallas as pl
from jax.experimental.pallas import tpu as pltpu
from jax.sharding import PartitionSpec as P

GROUPS = 16
LEVELS = (0.25, 0.5, 1.0, 2.0)
MESH = pl.DeviceIdType.MESH
F32, BF16 = jnp.float32, jnp.bfloat16


def cyclic_matrix(n):
    half = n // 2
    ev, od = np.eye(n)[0::2], np.eye(n)[1::2]
    r = lambda a, k: np.roll(a, k, 0)
    d = od - (0.5625 * (ev + r(ev, -1)) - 0.0625 * (r(ev, 1) + r(ev, -2)))
    s = ev + (0.28125 * (r(d, 1) + d) - 0.03125 * (r(d, 2) + r(d, -1)))
    return np.stack([s, d], 1).reshape(n, n) if half else None


def local_matrix(n):
    half = n // 2
    t = np.eye(n + 6)
    v, (a, b, c, f0, f1, g) = t[:n], t[n:]
    e = {j: v[2 * j] for j in range(half)}
    o = {j: v[2 * j + 1] for j in range(half)}
    e[-1], e[half], e[half + 1] = a, f0, f1
    d = {
        j: o[j] - 0.5625 * (e[j] + e[j + 1]) + 0.0625 * (e[j - 1] + e[j + 2])
        for j in range(half)
    }
    d[-1] = b - 0.5625 * e[0] + 0.0625 * e[1]
    d[-2] = c + 0.0625 * e[0]
    d[half] = g + 0.0625 * e[half - 1]
    out = np.zeros((n, n + 6))
    for j in range(half):
        out[2 * j] = e[j] + 0.28125 * (d[j - 1] + d[j]) - 0.03125 * (d[j - 2] + d[j + 1])
        out[2 * j + 1] = d[j]
    return out


def partials_low(row, n):
    a = row(n - 2)
    b = row(n - 1) - 0.5625 * a + 0.0625 * row(n - 4)
    c = row(n - 3) - 0.5625 * (row(n - 4) + a) + 0.0625 * row(n - 6)
    return a, b, c


def partials_high(row):
    f0, f1 = row(0), row(2)
    return f0, f1, row(1) - 0.5625 * (f0 + f1) + 0.0625 * row(4)


def split(value):
    hi = value.astype(BF16)
    return hi, (value - hi.astype(F32)).astype(BF16)


def dot2(left, right):
    dot = functools.partial(jnp.dot, preferred_element_type=F32)
    if left.dtype == BF16:
        hi, lo = split(right)
        return dot(left, hi) + dot(left, lo)
    hi, lo = split(left)
    return dot(hi, right) + dot(lo, right)


def kernel(
    n_row, n_col, grp, cut_hbm, map_hbm, p_ref, *refs
):
    weights, refs = refs[:6], refs[6:]
    out_hbm, mass_ref = refs[:2]
    ext, q, sx, su, u, sc, cb, part, slots, out_ref, cut_ref, map_ref = refs[2:14]
    held = refs[14:20]
    ws_ref, wy_ref, wu_ref, wx_ref, wc_ref, wz_ref = held
    in_sem, o_sem, w_sem, h_send, h_recv, g_send, g_recv, hop_sem = refs[20:]
    nx, ny, nz = p_ref.shape
    devices = n_row * n_col
    row, col = lax.axis_index("row"), lax.axis_index("col")
    me = row * n_col + col
    up_r, dn_r = lax.rem(row + 1, n_row), lax.rem(row + n_row - 1, n_row)
    up_c, dn_c = lax.rem(col + 1, n_col), lax.rem(col + n_col - 1, n_col)

    pieces = ((0, 8), (nx - 8, 8), (8, nx - 16))
    loads = []
    for i, (at, size) in enumerate(pieces):
        load = pltpu.make_async_copy(
            p_ref.at[pl.ds(at, size)], ext.at[pl.ds(at, size)], in_sem.at[i]
        )
        load.start()
        loads.append(load)

    fetched = []
    for i, (src, dst) in enumerate(
        zip((*weights, cut_hbm, map_hbm), (*held, cut_ref, map_ref), strict=True)
    ):
        fetch = pltpu.make_async_copy(src, dst, w_sem.at[i])
        fetch.start()
        fetched.append(fetch)

    def wrap(value, size):
        return lax.select(value >= size, value - size, value)

    def peers(visit):
        @pl.loop(1, n_col)
        def _(k):
            visit(row, wrap(col + k, n_col))

        @pl.loop(1, n_row)
        def _(j):
            other = wrap(row + j, n_row)

            @pl.loop(0, n_col)
            def _(k):
                visit(other, wrap(col + k, n_col))

    barrier = pltpu.get_barrier_semaphore()

    def greet(r, c):
        pl.semaphore_signal(barrier, inc=1, device_id=(r, c), device_id_type=MESH)

    for r, c in ((up_r, col), (dn_r, col), (row, up_c), (row, dn_c)):
        greet(r, c)
    along_col = max(n_col // 2 - 1, 1)
    hops = along_col + n_row // 2

    def call(k):
        aim = ((row, up_c), (row, dn_c)) if k < along_col else ((up_r, col), (dn_r, col))
        for to in aim:
            pl.semaphore_signal(hop_sem.at[k], inc=1, device_id=to, device_id_type=MESH)

    def relay(k):
        pl.semaphore_wait(hop_sem.at[k], 2)
        if k + 1 < hops:
            call(k + 1)


    sends = []

    def send(src, dst, to):
        i = len(sends)
        copy = pltpu.make_async_remote_copy(
            src_ref=src, dst_ref=dst, send_sem=h_send.at[i], recv_sem=h_recv.at[i],
            device_id=to, device_id_type=MESH,
        )
        copy.start()
        sends.append(copy)

    loads[0].wait()
    loads[1].wait()
    _, b, c = partials_low(lambda i: ext[i], nx)
    sx[0], sx[1] = b, c
    sx[2] = partials_high(lambda i: ext[i])[2]
    loads[2].wait()
    for fetch in fetched:
        fetch.wait()
    for g in range(nx // grp):
        at = pl.ds(g * grp, grp)
        got = dot2(ws_ref[...], ext[at].reshape(grp * ny, nz))
        su[:, at, :] = got.reshape(6, grp, nz)
    for d in range(4):
        for k in range(3):
            plane = (d % 2) * 3 + k
            x_row = lambda i: su[plane, pl.ds(i, 1), :]
            got = partials_low(x_row, nx) if d < 2 else partials_high(x_row)
            for i in range(3):
                sc[9 * d + 3 * i + k] = got[i]

    pl.semaphore_wait(barrier, 4)
    call(0)
    send(sx.at[pl.ds(0, 2)], ext.at[pl.ds(nx + 1, 2)], (up_r, col))
    send(sx.at[2], ext.at[nx + 5], (dn_r, col))
    send(ext.at[0], ext.at[nx + 3], (dn_r, col))
    send(su.at[pl.ds(0, 3)], u.at[pl.ds(0, 3)], (row, up_c))
    send(su.at[pl.ds(3, 3)], u.at[pl.ds(3, 3)], (row, dn_c))
    relay(0)
    for d in range(4):
        to = (up_r if d < 2 else dn_r, up_c if d % 2 == 0 else dn_c)
        send(sc.at[pl.ds(9 * d, 9)], cb.at[pl.ds(9 * d, 9)], to)
    send(ext.at[nx - 2], ext.at[nx], (up_r, col))
    send(ext.at[2], ext.at[nx + 4], (dn_r, col))

    for g in range(nx // grp):
        at = pl.ds(g * grp, grp)
        q[at] = dot2(wy_ref[...], ext[at].reshape(grp * ny, nz)).reshape(grp, ny, nz)
    relay(1)
    for copy in sends[3:5]:
        copy.wait_recv()
    relay(2)
    for g in range(nx // grp):
        at = pl.ds(g * grp, grp)
        more = dot2(wu_ref[...], u[:, at, :].reshape(6 * grp, nz))
        q[at] += more.reshape(grp, ny, nz)
    half = nx // 2
    relay(3)

    def x_lift(low, high):
        @pl.loop(0, ny // 8)
        def _(t):
            rows = pl.ds(pl.multiple_of(t * 8, 8), 8)
            far = {-1: nx, half: nx + 3, half + 1: nx + 4}
            first, last = max(low - 3, -1), min(high + 2, half + 1)
            e = {j: q[far.get(j, 2 * j), rows, :] for j in range(first, last + 1)}

            def detail(j):
                if j == -1:
                    return q[nx + 1, rows, :] - 0.5625 * e[0] + 0.0625 * e[1]
                if j == -2:
                    return q[nx + 2, rows, :] + 0.0625 * e[0]
                if j == half:
                    return q[nx + 5, rows, :] + 0.0625 * e[half - 1]
                odd = q[2 * j + 1, rows, :]
                return odd - 0.5625 * (e[j] + e[j + 1]) + 0.0625 * (e[j - 1] + e[j + 2])

            d = {j: detail(j) for j in range(low - 2, low + 1)}
            for j in range(low, high):
                d[j + 1] = detail(j + 1)
                near, wide = d[j - 1] + d[j], d[j - 2] + d[j + 1]
                ext[2 * j, rows, :] = e[j] + 0.28125 * near - 0.03125 * wide
                ext[2 * j + 1, rows, :] = d[j]

    zb = cut_ref.shape[2]
    width = nz // zb
    cuts = jnp.concatenate(
        [jnp.full((1, width), -cut_ref[0, 0, z], jnp.int32) for z in range(zb)], 1
    )
    scale = jnp.exp2(cuts.astype(F32))
    limits = [level * scale for level in LEVELS]
    odd = lambda axis: lax.broadcasted_iota(jnp.int32, (8, nz), axis) % 2
    mixed = (odd(0) + odd(1)) > 0

    def z_group(g, totals):
        at = pl.ds(g * grp, grp)
        made = dot2(ext[at].reshape(grp * ny, nz), wz_ref[...])
        out_ref[at] = made.reshape(grp, ny, nz)
        pltpu.make_async_copy(out_ref.at[at], out_hbm.at[at], o_sem.at[g]).start()
        totals = list(totals)
        for i in range(grp * ny // 8):
            size = jnp.abs(made[8 * i : 8 * i + 8])
            if (8 * i // ny) % 2 == 0:
                size = jnp.where(mixed, size, 0.0)
            for n, limit in enumerate(limits):
                totals[n] += jnp.maximum(size - limit, 0.0)
        return tuple(totals)

    groups = nx // grp
    totals = tuple(jnp.zeros((8, nz), F32) for _ in LEVELS)
    x_lift(grp // 2, half - grp // 2)
    totals = lax.fori_loop(1, groups - 1, z_group, totals)
    for k in range(4, hops):
        relay(k)
    for copy in sends[:3] + sends[5:]:
        copy.wait_recv()
    for copy in sends:
        copy.wait_send()
    edge = dot2(wx_ref[...], ext[pl.ds(nx, 6)].reshape(6 * ny, nz))
    edge += dot2(wc_ref[...], cb[...].reshape(-1, nz))
    q[pl.ds(nx, 6)] = edge.reshape(6, ny, nz)
    x_lift(0, grp // 2)
    x_lift(half - grp // 2, half)
    for g in (0, groups - 1):
        totals = z_group(g, totals)
    lane = lax.broadcasted_iota(jnp.int32, (1, 128), 1)
    line = jnp.zeros((1, 128), F32)
    cells = nx * ny * width
    n_lev = len(LEVELS)
    for z in range(zb):
        for n in range(n_lev):
            mass = jnp.sum(totals[n][:, z * width : (z + 1) * width], keepdims=True) / cells
            line += jnp.where(lane == n * GROUPS + map_ref[0, 0, z], mass, 0.0)
    part[...] = line
    slots[me] = line

    def spread(r, c):
        pltpu.make_async_remote_copy(
            src_ref=part, dst_ref=slots.at[me], send_sem=g_send.at[r * n_col + c],
            recv_sem=g_recv.at[me], device_id=(r, c), device_id_type=MESH,
        ).start()

    def gather(r, c):
        t = r * n_col + c
        pltpu.make_async_remote_copy(
            src_ref=part, dst_ref=slots.at[t], send_sem=g_send.at[t],
            recv_sem=g_recv.at[t], device_id=(r, c), device_id_type=MESH,
        ).wait()

    peers(spread)
    peers(gather)
    for g in range(groups):
        at = pl.ds(g * grp, grp)
        pltpu.make_async_copy(out_ref.at[at], out_hbm.at[at], o_sem.at[g]).wait()

    total = jnp.sum(slots[...], axis=0)
    mass_ref[...] = jnp.concatenate(
        [total[:, n * GROUPS : (n + 1) * GROUPS] for n in range(n_lev)], 0
    )


def deliver(c_hbm, m_hbm, out_hbm, mass_hbm, held, line, sems, m_sems):
    count = sems.shape[1]
    size = held.shape[0] // count
    piece = [pl.ds(i * size, size) for i in range(count)]
    copy = pltpu.make_async_copy
    ins = [copy(c_hbm.at[p], held.at[p], sems.at[0, i]) for i, p in enumerate(piece)]
    outs = [copy(held.at[p], out_hbm.at[p], sems.at[1, i]) for i, p in enumerate(piece)]
    ins.insert(1, copy(m_hbm, line, m_sems.at[0]))
    outs.insert(1, copy(line, mass_hbm, m_sems.at[1]))
    for c in ins:
        c.start()
    for c, o in zip(ins, outs, strict=True):
        c.wait()
        o.start()
    for o in outs:
        o.wait()


def solution(mesh):
    n_row, n_col = mesh.shape["row"], mesh.shape["col"]

    def shards(pressure, cut_exponent, group_map):
        nx, ny, nz = pressure.shape
        grp = 8
        devices = n_row * n_col
        local = local_matrix(ny)
        wy = np.kron(np.eye(grp), local[:, :ny])
        wu = np.einsum("xw,yk->xykw", np.eye(grp), local[:, ny:]).reshape(grp * ny, 6 * grp)
        eye = np.eye(ny)
        row = lambda i: eye[i]
        near = np.stack(partials_low(row, ny) + partials_high(row))
        ws = np.einsum("ky,xw->kxwy", near, np.eye(grp)).reshape(6 * grp, grp * ny)
        wx = np.kron(np.eye(6), local[:, :ny])
        wc = np.zeros((6, ny, 4, 9))
        for d in range(4):
            for i in range(3):
                for k in range(3):
                    wc[(d // 2) * 3 + i, :, d, 3 * i + k] = local[:, ny + (d % 2) * 3 + k]
        wc = wc.reshape(6 * ny, 36)
        weights = [jnp.asarray(w, BF16) for w in (ws, wy, wu, wx, wc, cyclic_matrix(nz).T)]
        vmem = pl.BlockSpec(memory_space=pltpu.VMEM)
        hbm = pl.BlockSpec(memory_space=pl.ANY)
        found = pl.pallas_call(
            functools.partial(kernel, n_row, n_col, grp),
            out_shape=(
                jax.ShapeDtypeStruct((nx, ny, nz), F32),
                jax.ShapeDtypeStruct((len(LEVELS), GROUPS), F32),
            ),
            in_specs=[hbm] * 9,
            out_specs=(hbm, vmem),
            scratch_shapes=[
                pltpu.VMEM((nx + 8, ny, nz), F32),
                pltpu.VMEM((nx + 6, ny, nz), F32),
                pltpu.VMEM((3, ny, nz), F32),
                pltpu.VMEM((6, nx, nz), F32),
                pltpu.VMEM((6, nx, nz), F32),
                pltpu.VMEM((36, 1, nz), F32),
                pltpu.VMEM((36, 1, nz), F32),
                pltpu.VMEM((1, 128), F32),
                pltpu.VMEM((devices, 1, 128), F32),
                pltpu.VMEM((nx, ny, nz), F32),
                pltpu.SMEM(cut_exponent.shape, jnp.int32),
                pltpu.SMEM(group_map.shape, jnp.int32),
                *(pltpu.VMEM(w.shape, BF16) for w in weights),
                pltpu.SemaphoreType.DMA((3,)),
                pltpu.SemaphoreType.DMA((nx // grp,)),
                pltpu.SemaphoreType.DMA((8,)),
                pltpu.SemaphoreType.DMA((11,)),
                pltpu.SemaphoreType.DMA((11,)),
                pltpu.SemaphoreType.DMA((devices,)),
                pltpu.SemaphoreType.DMA((devices,)),
                pltpu.SemaphoreType.REGULAR((n_col // 2 + n_row // 2,)),
            ],
            compiler_params=pltpu.CompilerParams(
                collective_id=0, has_side_effects=True, vmem_limit_bytes=62 * 2**20
            ),
        )(cut_exponent, group_map, pressure, *weights)
        coeffs, mass = pl.pallas_call(
            deliver,
            out_shape=tuple(jax.ShapeDtypeStruct(f.shape, F32) for f in found),
            in_specs=[hbm] * 2,
            out_specs=(hbm, hbm),
            scratch_shapes=[
                pltpu.VMEM((nx, ny, nz), F32),
                pltpu.VMEM(found[1].shape, F32),
                pltpu.SemaphoreType.DMA((2, 8)),
                pltpu.SemaphoreType.DMA((2,)),
            ],
            compiler_params=pltpu.CompilerParams(vmem_limit_bytes=62 * 2**20),
        )(*found)
        return coeffs, mass.T

    specs = P("row", "col", None)
    return jax.shard_map(
        shards, mesh=mesh, in_specs=(specs,) * 3, out_specs=(specs, P()), check_vma=False
    )
```

```python
import functools

import jax
import jax.numpy as jnp
import numpy as np
from jax import lax
from jax.experimental import pallas as pl
from jax.experimental.pallas import tpu as pltpu
from jax.sharding import PartitionSpec as P

GROUPS = 16
LEVELS = (0.25, 0.5, 1.0, 2.0)
MESH = pl.DeviceIdType.MESH
F32, BF16 = jnp.float32, jnp.bfloat16


def cyclic_matrix(n):
    half = n // 2
    ev, od = np.eye(n)[0::2], np.eye(n)[1::2]
    r = lambda a, k: np.roll(a, k, 0)
    d = od - (0.5625 * (ev + r(ev, -1)) - 0.0625 * (r(ev, 1) + r(ev, -2)))
    s = ev + (0.28125 * (r(d, 1) + d) - 0.03125 * (r(d, 2) + r(d, -1)))
    return np.stack([s, d], 1).reshape(n, n) if half else None


def local_matrix(n):
    half = n // 2
    t = np.eye(n + 6)
    v, (a, b, c, f0, f1, g) = t[:n], t[n:]
    e = {j: v[2 * j] for j in range(half)}
    o = {j: v[2 * j + 1] for j in range(half)}
    e[-1], e[half], e[half + 1] = a, f0, f1
    d = {
        j: o[j] - 0.5625 * (e[j] + e[j + 1]) + 0.0625 * (e[j - 1] + e[j + 2])
        for j in range(half)
    }
    d[-1] = b - 0.5625 * e[0] + 0.0625 * e[1]
    d[-2] = c + 0.0625 * e[0]
    d[half] = g + 0.0625 * e[half - 1]
    out = np.zeros((n, n + 6))
    for j in range(half):
        out[2 * j] = e[j] + 0.28125 * (d[j - 1] + d[j]) - 0.03125 * (d[j - 2] + d[j + 1])
        out[2 * j + 1] = d[j]
    return out


def partials_low(row, n):
    a = row(n - 2)
    b = row(n - 1) - 0.5625 * a + 0.0625 * row(n - 4)
    c = row(n - 3) - 0.5625 * (row(n - 4) + a) + 0.0625 * row(n - 6)
    return a, b, c


def partials_high(row):
    f0, f1 = row(0), row(2)
    return f0, f1, row(1) - 0.5625 * (f0 + f1) + 0.0625 * row(4)


def split(value):
    hi = value.astype(BF16)
    return hi, (value - hi.astype(F32)).astype(BF16)


def dot2(left, right):
    dot = functools.partial(jnp.dot, preferred_element_type=F32)
    if left.dtype == BF16:
        hi, lo = split(right)
        return dot(left, hi) + dot(left, lo)
    hi, lo = split(left)
    return dot(hi, right) + dot(lo, right)


def kernel(
    n_row, n_col, grp, cut_hbm, map_hbm, p_ref, *refs
):
    weights, refs = refs[:6], refs[6:]
    out_hbm, mass_ref = refs[:2]
    ext, q, sx, su, u, sc, cb, part, slots, out_ref, cut_ref, map_ref = refs[2:14]
    held = refs[14:20]
    ws_ref, wy_ref, wu_ref, wx_ref, wc_ref, wz_ref = held
    in_sem, o_sem, w_sem, h_send, h_recv, g_send, g_recv, hop_sem = refs[20:]
    nx, ny, nz = p_ref.shape
    devices = n_row * n_col
    row, col = lax.axis_index("row"), lax.axis_index("col")
    me = row * n_col + col
    up_r, dn_r = lax.rem(row + 1, n_row), lax.rem(row + n_row - 1, n_row)
    up_c, dn_c = lax.rem(col + 1, n_col), lax.rem(col + n_col - 1, n_col)

    def wrap(value, size):
        return lax.select(value >= size, value - size, value)

    def peers(visit):
        @pl.loop(1, n_row)
        def _(j):
            other = wrap(row + j, n_row)

            @pl.loop(0, n_col)
            def _(k):
                visit(other, wrap(col + k, n_col))

        @pl.loop(1, n_col)
        def _(k):
            visit(row, wrap(col + k, n_col))

    barrier = pltpu.get_barrier_semaphore()

    def greet(r, c):
        pl.semaphore_signal(barrier, inc=1, device_id=(r, c), device_id_type=MESH)

    for r, c in ((up_r, col), (dn_r, col), (row, up_c), (row, dn_c)):
        greet(r, c)
    pieces = ((0, 8), (nx - 8, 8), (8, nx - 16))
    loads = []
    for i, (at, size) in enumerate(pieces):
        load = pltpu.make_async_copy(
            p_ref.at[pl.ds(at, size)], ext.at[pl.ds(at, size)], in_sem.at[i]
        )
        load.start()
        loads.append(load)

    fetched = []
    for i, (src, dst) in enumerate(
        zip((*weights, cut_hbm, map_hbm), (*held, cut_ref, map_ref), strict=True)
    ):
        fetch = pltpu.make_async_copy(src, dst, w_sem.at[i])
        fetch.start()
        fetched.append(fetch)

    along_col = max(n_col // 2 - 1, 1)
    hops = along_col + n_row // 2

    def call(k):
        aim = ((row, up_c), (row, dn_c)) if k < along_col else ((up_r, col), (dn_r, col))
        for to in aim:
            pl.semaphore_signal(hop_sem.at[k], inc=1, device_id=to, device_id_type=MESH)

    def relay(k):
        pl.semaphore_wait(hop_sem.at[k], 2)
        if k + 1 < hops:
            call(k + 1)


    sends = []

    def send(src, dst, to):
        i = len(sends)
        copy = pltpu.make_async_remote_copy(
            src_ref=src, dst_ref=dst, send_sem=h_send.at[i], recv_sem=h_recv.at[i],
            device_id=to, device_id_type=MESH,
        )
        copy.start()
        sends.append(copy)

    loads[0].wait()
    loads[1].wait()
    _, b, c = partials_low(lambda i: ext[i], nx)
    sx[0], sx[1] = b, c
    sx[2] = partials_high(lambda i: ext[i])[2]
    loads[2].wait()
    for fetch in fetched:
        fetch.wait()
    for g in range(nx // grp):
        at = pl.ds(g * grp, grp)
        got = dot2(ws_ref[...], ext[at].reshape(grp * ny, nz))
        su[:, at, :] = got.reshape(6, grp, nz)
    for d in range(4):
        for k in range(3):
            plane = (d % 2) * 3 + k
            x_row = lambda i: su[plane, pl.ds(i, 1), :]
            got = partials_low(x_row, nx) if d < 2 else partials_high(x_row)
            for i in range(3):
                sc[9 * d + 3 * i + k] = got[i]

    pl.semaphore_wait(barrier, 4)
    call(0)
    send(sx.at[pl.ds(0, 2)], ext.at[pl.ds(nx + 1, 2)], (up_r, col))
    send(sx.at[2], ext.at[nx + 5], (dn_r, col))
    send(ext.at[nx - 2], ext.at[nx], (up_r, col))
    send(ext.at[0], ext.at[nx + 3], (dn_r, col))
    send(ext.at[2], ext.at[nx + 4], (dn_r, col))
    send(su.at[pl.ds(0, 3)], u.at[pl.ds(0, 3)], (row, up_c))
    send(su.at[pl.ds(3, 3)], u.at[pl.ds(3, 3)], (row, dn_c))
    relay(0)
    for d in range(4):
        to = (up_r if d < 2 else dn_r, up_c if d % 2 == 0 else dn_c)
        send(sc.at[pl.ds(9 * d, 9)], cb.at[pl.ds(9 * d, 9)], to)

    for g in range(nx // grp):
        at = pl.ds(g * grp, grp)
        q[at] = dot2(wy_ref[...], ext[at].reshape(grp * ny, nz)).reshape(grp, ny, nz)
    relay(1)
    for copy in sends[5:7]:
        copy.wait_recv()
    relay(2)
    for g in range(nx // grp):
        at = pl.ds(g * grp, grp)
        more = dot2(wu_ref[...], u[:, at, :].reshape(6 * grp, nz))
        q[at] += more.reshape(grp, ny, nz)
    half = nx // 2
    relay(3)

    def x_lift(low, high):
        @pl.loop(0, ny // 8)
        def _(t):
            rows = pl.ds(pl.multiple_of(t * 8, 8), 8)
            far = {-1: nx, half: nx + 3, half + 1: nx + 4}
            first, last = max(low - 3, -1), min(high + 2, half + 1)
            e = {j: q[far.get(j, 2 * j), rows, :] for j in range(first, last + 1)}

            def detail(j):
                if j == -1:
                    return q[nx + 1, rows, :] - 0.5625 * e[0] + 0.0625 * e[1]
                if j == -2:
                    return q[nx + 2, rows, :] + 0.0625 * e[0]
                if j == half:
                    return q[nx + 5, rows, :] + 0.0625 * e[half - 1]
                odd = q[2 * j + 1, rows, :]
                return odd - 0.5625 * (e[j] + e[j + 1]) + 0.0625 * (e[j - 1] + e[j + 2])

            d = {j: detail(j) for j in range(low - 2, low + 1)}
            for j in range(low, high):
                d[j + 1] = detail(j + 1)
                near, wide = d[j - 1] + d[j], d[j - 2] + d[j + 1]
                ext[2 * j, rows, :] = e[j] + 0.28125 * near - 0.03125 * wide
                ext[2 * j + 1, rows, :] = d[j]

    zb = cut_ref.shape[2]
    width = nz // zb
    cuts = jnp.concatenate(
        [jnp.full((1, width), -cut_ref[0, 0, z], jnp.int32) for z in range(zb)], 1
    )
    scale = jnp.exp2(cuts.astype(F32))
    limits = [level * scale for level in LEVELS]
    odd = lambda axis: lax.broadcasted_iota(jnp.int32, (8, nz), axis) % 2
    mixed = (odd(0) + odd(1)) > 0

    def z_group(g, totals):
        at = pl.ds(g * grp, grp)
        made = dot2(ext[at].reshape(grp * ny, nz), wz_ref[...])
        out_ref[at] = made.reshape(grp, ny, nz)
        pltpu.make_async_copy(out_ref.at[at], out_hbm.at[at], o_sem.at[g]).start()
        totals = list(totals)
        for i in range(grp * ny // 8):
            size = jnp.abs(made[8 * i : 8 * i + 8])
            if (8 * i // ny) % 2 == 0:
                size = jnp.where(mixed, size, 0.0)
            for n, limit in enumerate(limits):
                totals[n] += jnp.maximum(size - limit, 0.0)
        return tuple(totals)

    groups = nx // grp
    totals = tuple(jnp.zeros((8, nz), F32) for _ in LEVELS)
    x_lift(grp // 2, half - grp // 2)
    totals = lax.fori_loop(1, groups - 1, z_group, totals)
    for k in range(4, hops):
        relay(k)
    for copy in sends[:5] + sends[7:]:
        copy.wait_recv()
    for copy in sends:
        copy.wait_send()
    edge = dot2(wx_ref[...], ext[pl.ds(nx, 6)].reshape(6 * ny, nz))
    edge += dot2(wc_ref[...], cb[...].reshape(-1, nz))
    q[pl.ds(nx, 6)] = edge.reshape(6, ny, nz)
    x_lift(0, grp // 2)
    x_lift(half - grp // 2, half)
    for g in (0, groups - 1):
        totals = z_group(g, totals)
    lane = lax.broadcasted_iota(jnp.int32, (1, 128), 1)
    line = jnp.zeros((1, 128), F32)
    cells = nx * ny * width
    n_lev = len(LEVELS)
    for z in range(zb):
        for n in range(n_lev):
            mass = jnp.sum(totals[n][:, z * width : (z + 1) * width], keepdims=True) / cells
            line += jnp.where(lane == n * GROUPS + map_ref[0, 0, z], mass, 0.0)
    part[...] = line
    slots[me] = line

    def spread(r, c):
        pltpu.make_async_remote_copy(
            src_ref=part, dst_ref=slots.at[me], send_sem=g_send.at[r * n_col + c],
            recv_sem=g_recv.at[me], device_id=(r, c), device_id_type=MESH,
        ).start()

    def gather(r, c):
        t = r * n_col + c
        pltpu.make_async_remote_copy(
            src_ref=part, dst_ref=slots.at[t], send_sem=g_send.at[t],
            recv_sem=g_recv.at[t], device_id=(r, c), device_id_type=MESH,
        ).wait()

    peers(spread)
    peers(gather)
    for g in range(groups):
        at = pl.ds(g * grp, grp)
        pltpu.make_async_copy(out_ref.at[at], out_hbm.at[at], o_sem.at[g]).wait()

    total = jnp.sum(slots[...], axis=0)
    mass_ref[...] = jnp.concatenate(
        [total[:, n * GROUPS : (n + 1) * GROUPS] for n in range(n_lev)], 0
    )


def deliver(c_hbm, m_hbm, out_hbm, mass_hbm, held, line, sems, m_sems):
    count = sems.shape[1]
    size = held.shape[0] // count
    piece = [pl.ds(i * size, size) for i in range(count)]
    copy = pltpu.make_async_copy
    ins = [copy(c_hbm.at[p], held.at[p], sems.at[0, i]) for i, p in enumerate(piece)]
    outs = [copy(held.at[p], out_hbm.at[p], sems.at[1, i]) for i, p in enumerate(piece)]
    ins.insert(1, copy(m_hbm, line, m_sems.at[0]))
    outs.insert(1, copy(line, mass_hbm, m_sems.at[1]))
    for c in ins:
        c.start()
    for c, o in zip(ins, outs, strict=True):
        c.wait()
        o.start()
    for o in outs:
        o.wait()


def solution(mesh):
    n_row, n_col = mesh.shape["row"], mesh.shape["col"]

    def shards(pressure, cut_exponent, group_map):
        nx, ny, nz = pressure.shape
        grp = 8
        devices = n_row * n_col
        local = local_matrix(ny)
        wy = np.kron(np.eye(grp), local[:, :ny])
        wu = np.einsum("xw,yk->xykw", np.eye(grp), local[:, ny:]).reshape(grp * ny, 6 * grp)
        eye = np.eye(ny)
        row = lambda i: eye[i]
        near = np.stack(partials_low(row, ny) + partials_high(row))
        ws = np.einsum("ky,xw->kxwy", near, np.eye(grp)).reshape(6 * grp, grp * ny)
        wx = np.kron(np.eye(6), local[:, :ny])
        wc = np.zeros((6, ny, 4, 9))
        for d in range(4):
            for i in range(3):
                for k in range(3):
                    wc[(d // 2) * 3 + i, :, d, 3 * i + k] = local[:, ny + (d % 2) * 3 + k]
        wc = wc.reshape(6 * ny, 36)
        weights = [jnp.asarray(w, BF16) for w in (ws, wy, wu, wx, wc, cyclic_matrix(nz).T)]
        vmem = pl.BlockSpec(memory_space=pltpu.VMEM)
        hbm = pl.BlockSpec(memory_space=pl.ANY)
        found = pl.pallas_call(
            functools.partial(kernel, n_row, n_col, grp),
            out_shape=(
                jax.ShapeDtypeStruct((nx, ny, nz), F32),
                jax.ShapeDtypeStruct((len(LEVELS), GROUPS), F32),
            ),
            in_specs=[hbm] * 9,
            out_specs=(hbm, vmem),
            scratch_shapes=[
                pltpu.VMEM((nx + 8, ny, nz), F32),
                pltpu.VMEM((nx + 6, ny, nz), F32),
                pltpu.VMEM((3, ny, nz), F32),
                pltpu.VMEM((6, nx, nz), F32),
                pltpu.VMEM((6, nx, nz), F32),
                pltpu.VMEM((36, 1, nz), F32),
                pltpu.VMEM((36, 1, nz), F32),
                pltpu.VMEM((1, 128), F32),
                pltpu.VMEM((devices, 1, 128), F32),
                pltpu.VMEM((nx, ny, nz), F32),
                pltpu.SMEM(cut_exponent.shape, jnp.int32),
                pltpu.SMEM(group_map.shape, jnp.int32),
                *(pltpu.VMEM(w.shape, BF16) for w in weights),
                pltpu.SemaphoreType.DMA((3,)),
                pltpu.SemaphoreType.DMA((nx // grp,)),
                pltpu.SemaphoreType.DMA((8,)),
                pltpu.SemaphoreType.DMA((11,)),
                pltpu.SemaphoreType.DMA((11,)),
                pltpu.SemaphoreType.DMA((devices,)),
                pltpu.SemaphoreType.DMA((devices,)),
                pltpu.SemaphoreType.REGULAR((n_col // 2 + n_row // 2,)),
            ],
            compiler_params=pltpu.CompilerParams(
                collective_id=0, has_side_effects=True, vmem_limit_bytes=62 * 2**20
            ),
        )(cut_exponent, group_map, pressure, *weights)
        coeffs, mass = pl.pallas_call(
            deliver,
            out_shape=tuple(jax.ShapeDtypeStruct(f.shape, F32) for f in found),
            in_specs=[hbm] * 2,
            out_specs=(hbm, hbm),
            scratch_shapes=[
                pltpu.VMEM((nx, ny, nz), F32),
                pltpu.VMEM(found[1].shape, F32),
                pltpu.SemaphoreType.DMA((2, 8)),
                pltpu.SemaphoreType.DMA((2,)),
            ],
            compiler_params=pltpu.CompilerParams(vmem_limit_bytes=62 * 2**20),
        )(*found)
        return coeffs, mass.T

    specs = P("row", "col", None)
    return jax.shard_map(
        shards, mesh=mesh, in_specs=(specs,) * 3, out_specs=(specs, P()), check_vma=False
    )
```
